64 devices in a mesh: dp: 4 (over x, y), cp: 16 (over z, core).
Axes of the slice: x: 2, y: 2, z: 8, core: 2. Of those that a mesh axis runs over, the one named last changes fastest.
The devices are a block of a 4x4x8 slice.
Arguments:
- queries: bfloat16 [8, 6144, 4, 256], P('dp', 'cp'), parts along dimension 0
- keys: bfloat16 [8, 6144, 1, 256], P('dp', 'cp'), parts along dimension 0
- values: bfloat16 [8, 6144, 1, 256], P('dp', 'cp'), parts along dimension 0
- out_grad: bfloat16 [8, 6144, 4, 256], P('dp', 'cp'), parts along dimension 0
Outputs:
- output 1: bfloat16 [8, 6144, 4, 256], P('dp', 'cp'), parts along dimension 0
- output 2: float32 [8, 4, 6144], P('dp', None, 'cp'), parts along dimension 0
- output 3: bfloat16 [8, 6144, 4, 256], P('dp', 'cp'), parts along dimension 0
- output 4: bfloat16 [8, 6144, 1, 256], P('dp', 'cp'), parts along dimension 0
- output 5: bfloat16 [8, 6144, 1, 256], P('dp', 'cp'), parts along dimension 0
There are 4 independent parts. The reference program is written for one: setup_inputs(seed, part) draws one part's arguments, and reference() takes and returns one part's arrays. A program takes and returns all parts, laid end to end along the dimension named above; each array names one.
All inputs are finite; a program needn't handle non-finite values.
Results may differ from the reference program's by a relative error of at most 0.0185315.
Values are sent between devices in bfloat16 or wider.
A program may use at most 768 MiB of HBM per device.

```python
import jax
import jax.numpy as jnp
from jax import lax

BATCH = 2
SEQ = 6144
HEADS = 4
KV_HEADS = 1
HEAD = 256
QBLOCK = 128

RATIO = HEADS // KV_HEADS
SCALE = HEAD ** -0.5
NUM_BLOCKS = SEQ // QBLOCK


def setup_inputs(seed: int = 0, part: int = 0) -> dict:
    base_key = jax.random.fold_in(jax.random.key(seed), part)
    rng_keys = jax.random.split(base_key, 4)
    q_shape = (BATCH, SEQ, HEADS, HEAD)
    kv_shape = (BATCH, SEQ, KV_HEADS, HEAD)
    queries = jax.random.normal(rng_keys[0], q_shape, jnp.float32).astype(jnp.bfloat16)
    keys = jax.random.normal(rng_keys[1], kv_shape, jnp.float32).astype(jnp.bfloat16)
    values = jax.random.normal(rng_keys[2], kv_shape, jnp.float32).astype(jnp.bfloat16)
    out_grad = jax.random.normal(rng_keys[3], q_shape, jnp.float32).astype(jnp.bfloat16)
    return {"queries": queries, "keys": keys, "values": values, "out_grad": out_grad}


def reference(queries, keys, values, out_grad):
    keys_f = keys.astype(jnp.float32)
    values_f = values.astype(jnp.float32)
    key_pos = jnp.arange(SEQ)
    query_blocks = jnp.moveaxis(queries.reshape(BATCH, NUM_BLOCKS, QBLOCK, KV_HEADS, RATIO, HEAD), 1, 0)
    grad_blocks = jnp.moveaxis(out_grad.reshape(BATCH, NUM_BLOCKS, QBLOCK, KV_HEADS, RATIO, HEAD), 1, 0)

    def block_step(carry, block_in):
        grad_key, grad_value = carry
        block_idx, query_blk, grad_blk = block_in
        query_f = query_blk.astype(jnp.float32)
        grad_f = grad_blk.astype(jnp.float32)
        query_pos = block_idx * QBLOCK + jnp.arange(QBLOCK)
        causal = query_pos[:, None] >= key_pos[None, :]
        scores = jnp.einsum("bqgrd,bkgd->bgrqk", query_f, keys_f) * SCALE
        scores = jnp.where(causal, scores, -jnp.inf)
        row_max = jnp.max(scores, axis=-1, keepdims=True)
        row_lse = row_max + jnp.log(jnp.sum(jnp.exp(scores - row_max), axis=-1, keepdims=True))
        prob_mat = jnp.exp(scores - row_lse)
        prob_round = prob_mat.astype(jnp.bfloat16).astype(jnp.float32)
        out_blk = jnp.einsum("bgrqk,bkgd->bqgrd", prob_round, values_f).astype(jnp.bfloat16)
        delta = jnp.einsum("bqgrd,bqgrd->bgrq", grad_f, out_blk.astype(jnp.float32))
        grad_prob = jnp.einsum("bqgrd,bkgd->bgrqk", grad_f, values_f)
        grad_score = prob_mat * (grad_prob - delta[..., None])
        score_round = grad_score.astype(jnp.bfloat16).astype(jnp.float32)
        grad_query = jnp.einsum("bgrqk,bkgd->bqgrd", score_round, keys_f) * SCALE
        grad_key = grad_key + jnp.einsum("bgrqk,bqgrd->bkgd", score_round, query_f) * SCALE
        grad_value = grad_value + jnp.einsum("bgrqk,bqgrd->bkgd", prob_round, grad_f)
        return (grad_key, grad_value), (out_blk, row_lse[..., 0], grad_query.astype(jnp.bfloat16))

    zero_kv = jnp.zeros((BATCH, SEQ, KV_HEADS, HEAD), jnp.float32)
    carry_out, block_outs = lax.scan(block_step, (zero_kv, zero_kv), (jnp.arange(NUM_BLOCKS), query_blocks, grad_blocks))
    out_blocks, lse_blocks, dq_blocks = block_outs
    attn_out = jnp.moveaxis(out_blocks, 0, 1).reshape(BATCH, SEQ, HEADS, HEAD)
    row_lse = jnp.moveaxis(lse_blocks, 0, 3).reshape(BATCH, HEADS, SEQ)
    grad_query = jnp.moveaxis(dq_blocks, 0, 1).reshape(BATCH, SEQ, HEADS, HEAD)
    grad_key = carry_out[0].astype(jnp.bfloat16)
    grad_value = carry_out[1].astype(jnp.bfloat16)
    return attn_out, row_lse, grad_query, grad_key, grad_value
```

```python
import functools

import jax
import jax.numpy as jnp
from jax import lax
from jax.experimental import pallas as pl
from jax.experimental.pallas import tpu as pltpu
from jax.sharding import PartitionSpec as P

MESH = pl.DeviceIdType.MESH
LOG2E = 1.4426950408889634
LN2 = 0.6931471805599453
TILE = 256


def attention_kernel(n, scale, q_hbm, k_hbm, v_hbm, g_hbm, out_hbm, lse_hbm, dq_hbm, dk_hbm, dv_hbm,
                     k_all, v_all, turned, q_s, q_t, g_s, g_t, acc, run_m, run_l, delta, lse_s, out_s, dq_s, dk_s, dv_s,
                     dk_sum, dv_sum, dk_dn, dv_dn, dk_up, dv_up,
                     load_sem, swap_send, swap_recv, kv_up_send, kv_up_recv, kv_dn_send, kv_dn_recv,
                     dkv_dn_send, dkv_dn_recv, dkv_up_send, dkv_up_recv, store_sem, back_send, back_recv):
    heads, chunk, head_dim = q_s.shape
    half = chunk // 2
    tiles = chunk // TILE
    rank = lax.axis_index("cp")
    chip = rank // 2
    core = rank % 2
    other = 1 - core
    peer = 2 * chip + other
    above = 2 * ((chip + 1) % n) + core
    below = 2 * ((chip + n - 1) % n) + core
    mine = pl.ds(pl.multiple_of(core * half, half), half)
    theirs = pl.ds(pl.multiple_of(other * half, half), half)
    hops_up = (n // 2, n - 1 - n // 2)
    hops_dn = (n - 1 - n // 2, n // 2)
    kv_all = (k_all, v_all)
    sums = (dk_sum, dv_sum)
    from_up = (dk_dn, dv_dn)
    from_dn = (dk_up, dv_up)
    fold = scale * LOG2E

    def remote(src, dst, send_sem, recv_sem, device):
        return pltpu.make_async_remote_copy(src_ref=src, dst_ref=dst, send_sem=send_sem, recv_sem=recv_sem, device_id={"cp": device}, device_id_type=MESH)

    barrier = pltpu.get_barrier_semaphore()
    for device in (peer, above, below):
        pl.semaphore_signal(barrier, inc=1, device_id={"cp": device}, device_id_type=MESH)
    pl.semaphore_wait(barrier, 3)

    places = (k_all.at[chip, mine], v_all.at[chip, mine], q_s.at[:, mine], g_s.at[:, mine])
    sources = (k_hbm, v_hbm, q_hbm, g_hbm)
    swaps = [remote(sources[i].at[other], places[i], swap_send.at[i], swap_recv.at[i], peer) for i in range(4)]
    loads = [pltpu.make_async_copy(sources[i].at[core], places[i], load_sem.at[i]) for i in range(4)]
    for i in range(4):
        swaps[i].start()
        loads[i].start()

    def arrived(i):
        loads[i].wait()
        swaps[i].wait_recv()

    def kv_up(a, step, j):
        return remote(kv_all[a].at[j], kv_all[a].at[j], kv_up_send.at[a, step], kv_up_recv.at[a, step], above)

    def kv_dn(a, step, j):
        return remote(kv_all[a].at[j], kv_all[a].at[j], kv_dn_send.at[a, step], kv_dn_recv.at[a, step], below)

    def sends_up(a, step):
        return (chip < n - 1) & (chip - step >= 0) & (step < hops_up[a])

    def sends_dn(a, step):
        return ((chip + step) % n < hops_dn[a]) & (step < hops_dn[a])

    for a in range(2):
        arrived(a)

        @pl.when(sends_up(a, 0))
        def _():
            kv_up(a, 0, chip).start()

        @pl.when(sends_dn(a, 0))
        def _():
            kv_dn(a, 0, chip).start()

    def take_up(a, step):
        j = chip - 1 - step

        @pl.when((j >= 0) & (step < hops_up[a]))
        def _():
            kv_up(a, step, j).wait_recv()

            @pl.when(sends_up(a, step + 1))
            def _():
                kv_up(a, step + 1, j).start()

    def take_dn(a, step):
        j = (chip + 1 + step) % n

        @pl.when((j < hops_dn[a]) & (step < hops_dn[a]))
        def _():
            kv_dn(a, step, j).wait_recv()

            @pl.when(sends_dn(a, step + 1))
            def _():
                kv_dn(a, step + 1, j).start()

    def turn(ref, j):
        for i in range(tiles):
            turned[:, i * TILE:(i + 1) * TILE] = ref[j, i * TILE:(i + 1) * TILE, :].T

    def causal(rows, i):
        key = lax.broadcasted_iota(jnp.int32, (rows, TILE), 0)
        query = lax.broadcasted_iota(jnp.int32, (rows, TILE), 1) + i * TILE
        return key <= query

    def forward_chunk(j, diagonal):
        turn(v_all, j)

        def head(h, _):
            for i in range(tiles):
                cols = slice(i * TILE, (i + 1) * TILE)
                rows = (i + 1) * TILE if diagonal else chunk
                s = jnp.dot(k_all[j, :rows, :], q_t[h, :, cols], preferred_element_type=jnp.float32) * fold
                if diagonal:
                    s = jnp.where(causal(rows, i), s, -jnp.inf)
                    top = jnp.max(s, axis=0, keepdims=True)
                else:
                    old = run_m[h, :, cols]
                    top = jnp.maximum(old, jnp.max(s, axis=0, keepdims=True))
                p = jnp.exp2(s - top)
                total = jnp.sum(p, axis=0, keepdims=True)
                part = jnp.dot(turned[:, :rows], p.astype(jnp.bfloat16), preferred_element_type=jnp.float32)
                run_m[h, :, cols] = top
                if diagonal:
                    run_l[h, :, cols] = total
                    acc[h, :, cols] = part
                else:
                    alpha = jnp.exp2(old - top)
                    run_l[h, :, cols] = run_l[h, :, cols] * alpha + total
                    acc[h, :, cols] = acc[h, :, cols] * alpha + part
            return 0

        lax.fori_loop(0, heads, head, 0)

    arrived(2)

    def turn_q(h, _):
        for i in range(tiles):
            cols = slice(i * TILE, (i + 1) * TILE)
            q_t[h, :, cols] = q_s[h, cols, :].T
        return 0

    lax.fori_loop(0, heads, turn_q, 0)
    forward_chunk(chip, True)
    arrived(3)

    def turn_g(h, _):
        for i in range(tiles):
            cols = slice(i * TILE, (i + 1) * TILE)
            g_t[h, :, cols] = g_s[h, cols, :].T
        return 0

    lax.fori_loop(0, heads, turn_g, 0)

    def forward_pos(s, _):
        step = s // 2
        up = s % 2 == 0
        last = s == n - 2

        @pl.when(up)
        def _():
            take_up(0, step)
            take_up(1, step)

        @pl.when(jnp.logical_not(up))
        def _():
            take_dn(0, step)
            take_dn(1, step)

        @pl.when(last)
        def _():
            take_dn(1, step)

        j = jnp.where(up, chip - 1 - step, (chip + 1 + step) % n)
        valid = (j >= 0) & (j < chip) & (up | (j < hops_dn[0]))

        @pl.when(valid)
        def _():
            forward_chunk(j, False)

        return 0

    lax.fori_loop(0, n - 1, forward_pos, 0)

    def finish(h, _):
        for i in range(tiles):
            cols = slice(i * TILE, (i + 1) * TILE)
            total = run_l[h, :, cols]
            out = (acc[h, :, cols] / total).astype(jnp.bfloat16)
            acc[h, :, cols] = jnp.zeros((head_dim, TILE), jnp.float32)
            delta[h, :, cols] = jnp.sum(g_t[h, :, cols].astype(jnp.float32) * out.astype(jnp.float32), axis=0, keepdims=True)
            lse2 = run_m[h, :, cols] + jnp.log2(total)
            run_m[h, :, cols] = lse2
            lse_s[h, :, cols] = lse2 * LN2
            out_s[h, cols, :] = out.T
        return 0

    lax.fori_loop(0, heads, finish, 0)

    def give_back(i, src_mine, src_theirs, dst):
        swap = remote(src_theirs, dst.at[core], back_send.at[i], back_recv.at[i], peer)
        keep = pltpu.make_async_copy(src_mine, dst.at[core], store_sem.at[i])
        swap.start()
        keep.start()
        return swap, keep

    pending = [
        give_back(0, out_s.at[:, mine], out_s.at[:, theirs], out_hbm),
        give_back(1, lse_s.at[:, :, mine], lse_s.at[:, :, theirs], lse_hbm),
    ]

    def backward_chunk(j, diagonal):
        turn(k_all, j)
        dk_sum[j] = jnp.zeros((chunk, head_dim), jnp.float32)
        dv_sum[j] = jnp.zeros((chunk, head_dim), jnp.float32)

        def head(h, _):
            for i in range(tiles):
                cols = slice(i * TILE, (i + 1) * TILE)
                rows = (i + 1) * TILE if diagonal else chunk
                s = jnp.dot(k_all[j, :rows, :], q_t[h, :, cols], preferred_element_type=jnp.float32) * fold
                if diagonal:
                    s = jnp.where(causal(rows, i), s, -jnp.inf)
                p = jnp.exp2(s - run_m[h, :, cols])
                dp = jnp.dot(v_all[j, :rows, :], g_t[h, :, cols], preferred_element_type=jnp.float32)
                ds = (p * (dp - delta[h, :, cols])).astype(jnp.bfloat16)
                dv_sum[j, :rows, :] += jnp.dot(p.astype(jnp.bfloat16), g_s[h, cols, :], preferred_element_type=jnp.float32)
                dk_sum[j, :rows, :] += jnp.dot(ds, q_s[h, cols, :], preferred_element_type=jnp.float32)
                acc[h, :, cols] += jnp.dot(turned[:, :rows], ds, preferred_element_type=jnp.float32)
            return 0

        lax.fori_loop(0, heads, head, 0)

    def sum_dn(a, step, j):
        return remote(sums[a].at[j], from_up[a].at[step], dkv_dn_send.at[a, step], dkv_dn_recv.at[a, step], below)

    def sum_up(a, step, src):
        return remote(src, from_dn[a].at[step], dkv_up_send.at[a, step], dkv_up_recv.at[a, step], above)

    def gives_dn(a, step):
        return (chip - hops_up[a] + step >= 0) & (step < hops_up[a])

    def up_index(a, step):
        return (chip + hops_dn[a] - step + n) % n

    def gives_up(a, step):
        j = up_index(a, step)
        return (j < hops_dn[a]) & (j != chip) & (step < hops_dn[a])

    def add_in(a, j, part):
        sums[a][j] = sums[a][j] + part

    def pass_dn(a, step):
        @pl.when(gives_dn(a, step))
        def _():
            j = chip - hops_up[a] + step

            before = jnp.maximum(step - 1, 0)

            @pl.when((step >= 1) & (chip < n - 1))
            def _():
                sum_dn(a, before, j).wait_recv()
                add_in(a, j, from_up[a][before])

            sum_dn(a, step, j).start()

    def pass_up(a, step):
        @pl.when(gives_up(a, step))
        def _():
            j = up_index(a, step)
            before = jnp.maximum(step - 1, 0)

            @pl.when(step >= 1)
            def _():
                sum_up(a, before, sums[a].at[j]).wait_recv()

            @pl.when(j < chip)
            def _():
                @pl.when(step >= 1)
                def _():
                    add_in(a, j, from_dn[a][before])

                sum_up(a, step, sums[a].at[j]).start()

            @pl.when(j > chip)
            def _():
                sum_up(a, step, from_dn[a].at[before]).start()

    def backward_pos(s, _):
        step = jnp.maximum(s - 1, 0) // 2
        first = s == 0
        down = s % 2 == 1
        near = chip - hops_up[1] + step
        far = up_index(0, step)
        j = jnp.where(first, chip - n // 2, jnp.where(down, near, far))
        valid = (j >= 0) & (j < chip) & (first | down | (j < hops_dn[0]))

        @pl.when(valid)
        def _():
            backward_chunk(j, False)

        @pl.when(first)
        def _():
            pass_dn(0, 0)
            pass_up(1, 0)

        @pl.when(down)
        def _():
            pass_dn(0, step + 1)
            pass_dn(1, step)

        @pl.when(jnp.logical_not(first | down))
        def _():
            pass_up(0, step)
            pass_up(1, step + 1)

        @pl.when(s == n // 2 - 1)
        def _():
            backward_chunk(chip, True)

        return 0

    lax.fori_loop(0, n - 1, backward_pos, 0)

    def finish_q(h, _):
        for i in range(tiles):
            cols = slice(i * TILE, (i + 1) * TILE)
            dq_s[h, cols, :] = (acc[h, :, cols] * scale).astype(jnp.bfloat16).T
        return 0

    lax.fori_loop(0, heads, finish_q, 0)
    pending.append(give_back(2, dq_s.at[:, mine], dq_s.at[:, theirs], dq_hbm))

    for a in range(2):
        @pl.when(chip < hops_dn[a])
        def _():
            sum_up(a, hops_dn[a] - 1, sums[a].at[chip]).wait_recv()
            add_in(a, chip, from_dn[a][hops_dn[a] - 1])

        @pl.when(chip < n - 1)
        def _():
            sum_dn(a, hops_up[a] - 1, chip).wait_recv()
            add_in(a, chip, from_up[a][hops_up[a] - 1])

        if a == 0:
            dk_s[...] = (dk_sum[chip] * scale).astype(jnp.bfloat16)
            pending.append(give_back(3, dk_s.at[mine], dk_s.at[theirs], dk_hbm))
        else:
            dv_s[...] = dv_sum[chip].astype(jnp.bfloat16)
            pending.append(give_back(4, dv_s.at[mine], dv_s.at[theirs], dv_hbm))

    for i in range(4):
        swaps[i].wait_send()
    for a in range(2):
        for step in range(hops_up[a]):
            @pl.when(sends_up(a, step))
            def _():
                kv_up(a, step, 0).wait_send()

            @pl.when(gives_dn(a, step))
            def _():
                sum_dn(a, step, 0).wait_send()

        for step in range(hops_dn[a]):
            @pl.when(sends_dn(a, step))
            def _():
                kv_dn(a, step, 0).wait_send()

            @pl.when(gives_up(a, step))
            def _():
                sum_up(a, step, sums[a].at[0]).wait_send()

    for swap, keep in pending:
        keep.wait()
        swap.wait()


def solution(mesh):
    chips = mesh.shape["cp"] // 2

    def attention_shard(queries, keys, values, out_grad):
        batch, tokens, heads, head_dim = queries.shape
        chunk = 2 * tokens
        half = chips // 2
        bf16, f32 = jnp.bfloat16, jnp.float32
        q = jnp.transpose(queries, (0, 2, 1, 3))
        g = jnp.transpose(out_grad, (0, 2, 1, 3))
        k = keys.reshape(batch, tokens, head_dim)
        v = values.reshape(batch, tokens, head_dim)
        any_spec = pl.BlockSpec(memory_space=pl.ANY)
        dma = pltpu.SemaphoreType.DMA
        out, lse, dq, dk, dv = pl.pallas_call(
            functools.partial(attention_kernel, chips, head_dim ** -0.5),
            out_shape=(
                jax.ShapeDtypeStruct(q.shape, bf16),
                jax.ShapeDtypeStruct((batch, heads, 1, tokens), f32),
                jax.ShapeDtypeStruct(q.shape, bf16),
                jax.ShapeDtypeStruct(k.shape, bf16),
                jax.ShapeDtypeStruct(k.shape, bf16),
            ),
            in_specs=[any_spec] * 4,
            out_specs=(any_spec,) * 5,
            scratch_shapes=[
                pltpu.VMEM((chips, chunk, head_dim), bf16),
                pltpu.VMEM((chips, chunk, head_dim), bf16),
                pltpu.VMEM((head_dim, chunk), bf16),
                pltpu.VMEM((heads, chunk, head_dim), bf16),
                pltpu.VMEM((heads, head_dim, chunk), bf16),
                pltpu.VMEM((heads, chunk, head_dim), bf16),
                pltpu.VMEM((heads, head_dim, chunk), bf16),
                pltpu.VMEM((heads, head_dim, chunk), f32),
                pltpu.VMEM((heads, 1, chunk), f32),
                pltpu.VMEM((heads, 1, chunk), f32),
                pltpu.VMEM((heads, 1, chunk), f32),
                pltpu.VMEM((heads, 1, chunk), f32),
                pltpu.VMEM((heads, chunk, head_dim), bf16),
                pltpu.VMEM((heads, chunk, head_dim), bf16),
                pltpu.VMEM((chunk, head_dim), bf16),
                pltpu.VMEM((chunk, head_dim), bf16),
                pltpu.VMEM((chips, chunk, head_dim), f32),
                pltpu.VMEM((chips, chunk, head_dim), f32),
                pltpu.VMEM((half, chunk, head_dim), f32),
                pltpu.VMEM((half - 1, chunk, head_dim), f32),
                pltpu.VMEM((half - 1, chunk, head_dim), f32),
                pltpu.VMEM((half, chunk, head_dim), f32),
                dma((4,)), dma((4,)), dma((4,)),
                dma((2, half)), dma((2, half)), dma((2, half)), dma((2, half)),
                dma((2, half)), dma((2, half)), dma((2, half)), dma((2, half)),
                dma((5,)), dma((5,)), dma((5,)),
            ],
            compiler_params=pltpu.CompilerParams(collective_id=0, has_side_effects=True, vmem_limit_bytes=67043328),
            name="ring_attention",
        )(q, k, v, g)
        back = (0, 2, 1, 3)
        return (
            jnp.transpose(out, back),
            lse.reshape(batch, heads, tokens),
            jnp.transpose(dq, back),
            dk.reshape(keys.shape),
            dv.reshape(values.shape),
        )

    seq_spec = P("dp", "cp")
    return jax.shard_map(attention_shard, mesh=mesh, in_specs=(seq_spec,) * 4, out_specs=(seq_spec, P("dp", None, "cp"), seq_spec, seq_spec, seq_spec), check_vma=False)
```

```python
import functools

import jax
import jax.numpy as jnp
from jax import lax
from jax.experimental import pallas as pl
from jax.experimental.pallas import tpu as pltpu
from jax.sharding import PartitionSpec as P

MESH = pl.DeviceIdType.MESH
LOG2E = 1.4426950408889634
LN2 = 0.6931471805599453
TILE = 256


def attention_kernel(n, scale, q_hbm, k_hbm, v_hbm, g_hbm, out_hbm, lse_hbm, dq_hbm, dk_hbm, dv_hbm,
                     k_all, v_all, turned, q_s, q_t, g_s, g_t, acc, run_m, run_l, delta, lse_s, out_s, dq_s, dk_s, dv_s,
                     dk_sum, dv_sum, dk_dn, dv_dn, dk_up, dv_up,
                     load_sem, swap_send, swap_recv, kv_up_send, kv_up_recv, kv_dn_send, kv_dn_recv,
                     dkv_dn_send, dkv_dn_recv, dkv_up_send, dkv_up_recv, store_sem, back_send, back_recv, go_sem):
    heads, chunk, head_dim = q_s.shape
    half = chunk // 2
    tiles = chunk // TILE
    rank = lax.axis_index("cp")
    chip = rank // 2
    core = rank % 2
    other = 1 - core
    peer = 2 * chip + other
    above = 2 * ((chip + 1) % n) + core
    below = 2 * ((chip + n - 1) % n) + core
    mine = pl.ds(pl.multiple_of(core * half, half), half)
    theirs = pl.ds(pl.multiple_of(other * half, half), half)
    hops_up = (n // 2, n - 1 - n // 2)
    hops_dn = (n - 1 - n // 2, n // 2)
    kv_all = (k_all, v_all)
    sums = (dk_sum, dv_sum)
    from_up = (dk_dn, dv_dn)
    from_dn = (dk_up, dv_up)
    fold = scale * LOG2E

    def remote(src, dst, send_sem, recv_sem, device):
        return pltpu.make_async_remote_copy(src_ref=src, dst_ref=dst, send_sem=send_sem, recv_sem=recv_sem, device_id={"cp": device}, device_id_type=MESH)

    barrier = pltpu.get_barrier_semaphore()
    for device in (peer, above, below):
        pl.semaphore_signal(barrier, inc=1, device_id={"cp": device}, device_id_type=MESH)
    pl.semaphore_wait(barrier, 3)

    places = (k_all.at[chip, mine], v_all.at[chip, mine], q_s.at[:, mine], g_s.at[:, mine])
    sources = (k_hbm, v_hbm, q_hbm, g_hbm)
    swaps = [remote(sources[i].at[other], places[i], swap_send.at[i], swap_recv.at[i], peer) for i in range(4)]
    loads = [pltpu.make_async_copy(sources[i].at[core], places[i], load_sem.at[i]) for i in range(4)]
    for i in range(4):
        swaps[i].start()
        loads[i].start()

    def arrived(i):
        loads[i].wait()
        swaps[i].wait_recv()

    def kv_up(a, step, j):
        return remote(kv_all[a].at[j], kv_all[a].at[j], kv_up_send.at[a, step], kv_up_recv.at[a, step], above)

    def kv_dn(a, step, j):
        return remote(kv_all[a].at[j], kv_all[a].at[j], kv_dn_send.at[a, step], kv_dn_recv.at[a, step], below)

    def sends_up(a, step):
        return (chip < n - 1) & (chip - step >= 0) & (step < hops_up[a])

    def sends_dn(a, step):
        return ((chip + step) % n < hops_dn[a]) & (step < hops_dn[a])

    def send_own(a):
        @pl.when(sends_up(a, 0))
        def _():
            kv_up(a, 0, chip).start()

        @pl.when(sends_dn(a, 0))
        def _():
            kv_dn(a, 0, chip).start()

    def sent_all():
        for a in range(2):
            for step in range(hops_up[a]):
                @pl.when(sends_up(a, step))
                def _():
                    kv_up(a, step, 0).wait_send()

            for step in range(hops_dn[a]):
                @pl.when(sends_dn(a, step))
                def _():
                    kv_dn(a, step, 0).wait_send()

    for a in range(2):
        arrived(a)

        @pl.when(core == 0)
        def _():
            send_own(a)

    def take_up(a, step):
        j = chip - 1 - step

        @pl.when((j >= 0) & (step < hops_up[a]))
        def _():
            kv_up(a, step, j).wait_recv()

            @pl.when(sends_up(a, step + 1))
            def _():
                kv_up(a, step + 1, j).start()

    def take_dn(a, step):
        j = (chip + 1 + step) % n

        @pl.when((j < hops_dn[a]) & (step < hops_dn[a]))
        def _():
            kv_dn(a, step, j).wait_recv()

            @pl.when(sends_dn(a, step + 1))
            def _():
                kv_dn(a, step + 1, j).start()

    def turn(ref, j):
        for i in range(tiles):
            turned[:, i * TILE:(i + 1) * TILE] = ref[j, i * TILE:(i + 1) * TILE, :].T

    def causal(rows, i):
        key = lax.broadcasted_iota(jnp.int32, (rows, TILE), 0)
        query = lax.broadcasted_iota(jnp.int32, (rows, TILE), 1) + i * TILE
        return key <= query

    def forward_chunk(j, diagonal):
        turn(v_all, j)

        def head(h, _):
            for i in range(tiles):
                cols = slice(i * TILE, (i + 1) * TILE)
                rows = (i + 1) * TILE if diagonal else chunk
                s = jnp.dot(k_all[j, :rows, :], q_t[h, :, cols], preferred_element_type=jnp.float32) * fold
                if diagonal:
                    s = jnp.where(causal(rows, i), s, -jnp.inf)
                    top = jnp.max(s, axis=0, keepdims=True)
                else:
                    old = run_m[h, :, cols]
                    top = jnp.maximum(old, jnp.max(s, axis=0, keepdims=True))
                p = jnp.exp2(s - top)
                total = jnp.sum(p, axis=0, keepdims=True)
                part = jnp.dot(turned[:, :rows], p.astype(jnp.bfloat16), preferred_element_type=jnp.float32)
                run_m[h, :, cols] = top
                if diagonal:
                    run_l[h, :, cols] = total
                    acc[h, :, cols] = part
                else:
                    alpha = jnp.exp2(old - top)
                    run_l[h, :, cols] = run_l[h, :, cols] * alpha + total
                    acc[h, :, cols] = acc[h, :, cols] * alpha + part
            return 0

        lax.fori_loop(0, heads, head, 0)

    arrived(2)

    def turn_q(h, _):
        for i in range(tiles):
            cols = slice(i * TILE, (i + 1) * TILE)
            q_t[h, :, cols] = q_s[h, cols, :].T
        return 0

    lax.fori_loop(0, heads, turn_q, 0)
    forward_chunk(chip, True)
    arrived(3)

    def turn_g(h, _):
        for i in range(tiles):
            cols = slice(i * TILE, (i + 1) * TILE)
            g_t[h, :, cols] = g_s[h, cols, :].T
        return 0

    lax.fori_loop(0, heads, turn_g, 0)

    @pl.when(core == 1)
    def _():
        pl.semaphore_wait(go_sem, 1)
        send_own(0)
        send_own(1)

    def forward_pos(s, _):
        step = s // 2
        up = s % 2 == 0
        last = s == n - 2

        @pl.when(up)
        def _():
            take_up(0, step)
            take_up(1, step)

        @pl.when(jnp.logical_not(up))
        def _():
            take_dn(0, step)
            take_dn(1, step)

        @pl.when(last)
        def _():
            take_dn(1, step)
            sent_all()

            @pl.when(core == 0)
            def _():
                pl.semaphore_signal(go_sem, inc=1, device_id={"cp": peer}, device_id_type=MESH)

        j = jnp.where(up, chip - 1 - step, (chip + 1 + step) % n)
        valid = (j >= 0) & (j < chip) & (up | (j < hops_dn[0]))

        @pl.when(valid)
        def _():
            forward_chunk(j, False)

        return 0

    lax.fori_loop(0, n - 1, forward_pos, 0)

    def finish(h, _):
        for i in range(tiles):
            cols = slice(i * TILE, (i + 1) * TILE)
            total = run_l[h, :, cols]
            out = (acc[h, :, cols] / total).astype(jnp.bfloat16)
            acc[h, :, cols] = jnp.zeros((head_dim, TILE), jnp.float32)
            delta[h, :, cols] = jnp.sum(g_t[h, :, cols].astype(jnp.float32) * out.astype(jnp.float32), axis=0, keepdims=True)
            lse2 = run_m[h, :, cols] + jnp.log2(total)
            run_m[h, :, cols] = lse2
            lse_s[h, :, cols] = lse2 * LN2
            out_s[h, cols, :] = out.T
        return 0

    lax.fori_loop(0, heads, finish, 0)

    def give_back(i, src_mine, src_theirs, dst):
        swap = remote(src_theirs, dst.at[core], back_send.at[i], back_recv.at[i], peer)
        keep = pltpu.make_async_copy(src_mine, dst.at[core], store_sem.at[i])
        swap.start()
        keep.start()
        return swap, keep

    pending = [
        give_back(0, out_s.at[:, mine], out_s.at[:, theirs], out_hbm),
        give_back(1, lse_s.at[:, :, mine], lse_s.at[:, :, theirs], lse_hbm),
    ]

    def backward_chunk(j, diagonal):
        turn(k_all, j)
        dk_sum[j] = jnp.zeros((chunk, head_dim), jnp.float32)
        dv_sum[j] = jnp.zeros((chunk, head_dim), jnp.float32)

        def head(h, _):
            for i in range(tiles):
                cols = slice(i * TILE, (i + 1) * TILE)
                rows = (i + 1) * TILE if diagonal else chunk
                s = jnp.dot(k_all[j, :rows, :], q_t[h, :, cols], preferred_element_type=jnp.float32) * fold
                if diagonal:
                    s = jnp.where(causal(rows, i), s, -jnp.inf)
                p = jnp.exp2(s - run_m[h, :, cols])
                dp = jnp.dot(v_all[j, :rows, :], g_t[h, :, cols], preferred_element_type=jnp.float32)
                ds = (p * (dp - delta[h, :, cols])).astype(jnp.bfloat16)
                dv_sum[j, :rows, :] += jnp.dot(p.astype(jnp.bfloat16), g_s[h, cols, :], preferred_element_type=jnp.float32)
                dk_sum[j, :rows, :] += jnp.dot(ds, q_s[h, cols, :], preferred_element_type=jnp.float32)
                acc[h, :, cols] += jnp.dot(turned[:, :rows], ds, preferred_element_type=jnp.float32)
            return 0

        lax.fori_loop(0, heads, head, 0)

    def sum_dn(a, step, j):
        return remote(sums[a].at[j], from_up[a].at[step], dkv_dn_send.at[a, step], dkv_dn_recv.at[a, step], below)

    def sum_up(a, step, src):
        return remote(src, from_dn[a].at[step], dkv_up_send.at[a, step], dkv_up_recv.at[a, step], above)

    wide = n // 2

    def gives_dn(a, step):
        skip = (a == 0) & (step == 0) & (chip == n - 1)
        return (chip - hops_up[a] + step >= 0) & (step < hops_up[a]) & jnp.logical_not(skip)

    def gets_dn(a, step):
        skip = (a == 0) & (step == 1) & (chip == n - 2)
        return (step >= 1) & (chip < n - 1) & jnp.logical_not(skip)

    def up_index(step):
        return (chip + wide - step + n) % n

    def gives_up(a, step):
        j = up_index(step)
        return (j < wide) & (j != chip) & (step < wide) & ((a == 1) | (step >= 1) | (chip == n - 1))

    def gets_up(a, step):
        return (step >= 2 - a) | ((step >= 1) & (up_index(step) > chip))

    def add_in(a, j, part):
        sums[a][j] = sums[a][j] + part

    def pass_dn(a, step):
        @pl.when(gives_dn(a, step))
        def _():
            j = chip - hops_up[a] + step

            before = jnp.maximum(step - 1, 0)

            @pl.when(gets_dn(a, step))
            def _():
                sum_dn(a, before, j).wait_recv()
                add_in(a, j, from_up[a][before])

            sum_dn(a, step, j).start()

    def pass_up(a, step):
        @pl.when(gives_up(a, step))
        def _():
            j = up_index(step)
            before = jnp.maximum(step - 1, 0)

            @pl.when(gets_up(a, step))
            def _():
                sum_up(a, before, sums[a].at[j]).wait_recv()

            @pl.when(j < chip)
            def _():
                @pl.when(gets_up(a, step))
                def _():
                    add_in(a, j, from_dn[a][before])

                sum_up(a, step, sums[a].at[j]).start()

            @pl.when(j > chip)
            def _():
                sum_up(a, step, from_dn[a].at[before]).start()

    def backward_pos(s, _):
        step = jnp.maximum(s - 1, 0) // 2
        first = s == 0
        down = s % 2 == 1
        near = chip - hops_up[1] + step
        far = up_index(step + 1)
        j = jnp.where(first, chip - n // 2, jnp.where(down, near, far))
        valid = (j >= 0) & (j < chip) & (first | down | (j < wide))

        @pl.when(valid)
        def _():
            backward_chunk(j, False)

        @pl.when(first)
        def _():
            pass_dn(0, 0)
            pass_up(0, 0)
            pass_up(1, 0)

        @pl.when(down)
        def _():
            pass_dn(0, step + 1)
            pass_dn(1, step)

        @pl.when(jnp.logical_not(first | down))
        def _():
            pass_up(0, step + 1)
            pass_up(1, step + 1)

        @pl.when(s == n // 2 - 1)
        def _():
            backward_chunk(chip, True)

        return 0

    lax.fori_loop(0, n - 1, backward_pos, 0)

    def finish_q(h, _):
        for i in range(tiles):
            cols = slice(i * TILE, (i + 1) * TILE)
            dq_s[h, cols, :] = (acc[h, :, cols] * scale).astype(jnp.bfloat16).T
        return 0

    lax.fori_loop(0, heads, finish_q, 0)
    pending.append(give_back(2, dq_s.at[:, mine], dq_s.at[:, theirs], dq_hbm))

    for a in range(2):
        @pl.when(chip < wide)
        def _():
            sum_up(a, wide - 1, sums[a].at[chip]).wait_recv()
            add_in(a, chip, from_dn[a][wide - 1])

        @pl.when(chip < n - 1)
        def _():
            sum_dn(a, hops_up[a] - 1, chip).wait_recv()
            add_in(a, chip, from_up[a][hops_up[a] - 1])

        if a == 0:
            dk_s[...] = (dk_sum[chip] * scale).astype(jnp.bfloat16)
            pending.append(give_back(3, dk_s.at[mine], dk_s.at[theirs], dk_hbm))
        else:
            dv_s[...] = dv_sum[chip].astype(jnp.bfloat16)
            pending.append(give_back(4, dv_s.at[mine], dv_s.at[theirs], dv_hbm))

    for i in range(4):
        swaps[i].wait_send()
    for a in range(2):
        for step in range(hops_up[a]):
            @pl.when(gives_dn(a, step))
            def _():
                sum_dn(a, step, 0).wait_send()

        for step in range(wide):
            @pl.when(gives_up(a, step))
            def _():
                sum_up(a, step, sums[a].at[0]).wait_send()

    for swap, keep in pending:
        keep.wait()
        swap.wait()


def solution(mesh):
    chips = mesh.shape["cp"] // 2

    def attention_shard(queries, keys, values, out_grad):
        batch, tokens, heads, head_dim = queries.shape
        chunk = 2 * tokens
        half = chips // 2
        bf16, f32 = jnp.bfloat16, jnp.float32
        q = jnp.transpose(queries, (0, 2, 1, 3))
        g = jnp.transpose(out_grad, (0, 2, 1, 3))
        k = keys.reshape(batch, tokens, head_dim)
        v = values.reshape(batch, tokens, head_dim)
        any_spec = pl.BlockSpec(memory_space=pl.ANY)
        dma = pltpu.SemaphoreType.DMA
        out, lse, dq, dk, dv = pl.pallas_call(
            functools.partial(attention_kernel, chips, head_dim ** -0.5),
            out_shape=(
                jax.ShapeDtypeStruct(q.shape, bf16),
                jax.ShapeDtypeStruct((batch, heads, 1, tokens), f32),
                jax.ShapeDtypeStruct(q.shape, bf16),
                jax.ShapeDtypeStruct(k.shape, bf16),
                jax.ShapeDtypeStruct(k.shape, bf16),
            ),
            in_specs=[any_spec] * 4,
            out_specs=(any_spec,) * 5,
            scratch_shapes=[
                pltpu.VMEM((chips, chunk, head_dim), bf16),
                pltpu.VMEM((chips, chunk, head_dim), bf16),
                pltpu.VMEM((head_dim, chunk), bf16),
                pltpu.VMEM((heads, chunk, head_dim), bf16),
                pltpu.VMEM((heads, head_dim, chunk), bf16),
                pltpu.VMEM((heads, chunk, head_dim), bf16),
                pltpu.VMEM((heads, head_dim, chunk), bf16),
                pltpu.VMEM((heads, head_dim, chunk), f32),
                pltpu.VMEM((heads, 1, chunk), f32),
                pltpu.VMEM((heads, 1, chunk), f32),
                pltpu.VMEM((heads, 1, chunk), f32),
                pltpu.VMEM((heads, 1, chunk), f32),
                pltpu.VMEM((heads, chunk, head_dim), bf16),
                pltpu.VMEM((heads, chunk, head_dim), bf16),
                pltpu.VMEM((chunk, head_dim), bf16),
                pltpu.VMEM((chunk, head_dim), bf16),
                pltpu.VMEM((chips, chunk, head_dim), f32),
                pltpu.VMEM((chips, chunk, head_dim), f32),
                pltpu.VMEM((half, chunk, head_dim), f32),
                pltpu.VMEM((half - 1, chunk, head_dim), f32),
                pltpu.VMEM((half, chunk, head_dim), f32),
                pltpu.VMEM((half, chunk, head_dim), f32),
                dma((4,)), dma((4,)), dma((4,)),
                dma((2, half)), dma((2, half)), dma((2, half)), dma((2, half)),
                dma((2, half)), dma((2, half)), dma((2, half)), dma((2, half)),
                dma((5,)), dma((5,)), dma((5,)), pltpu.SemaphoreType.REGULAR,
            ],
            compiler_params=pltpu.CompilerParams(collective_id=0, has_side_effects=True, vmem_limit_bytes=67043328),
            name="ring_attention",
        )(q, k, v, g)
        back = (0, 2, 1, 3)
        return (
            jnp.transpose(out, back),
            lse.reshape(batch, heads, tokens),
            jnp.transpose(dq, back),
            dk.reshape(keys.shape),
            dv.reshape(values.shape),
        )

    seq_spec = P("dp", "cp")
    return jax.shard_map(attention_shard, mesh=mesh, in_specs=(seq_spec,) * 4, out_specs=(seq_spec, P("dp", None, "cp"), seq_spec, seq_spec, seq_spec), check_vma=False)
```

```python
import functools

import jax
import jax.numpy as jnp
from jax import lax
from jax.experimental import pallas as pl
from jax.experimental.pallas import tpu as pltpu
from jax.sharding import PartitionSpec as P

MESH = pl.DeviceIdType.MESH
LOG2E = 1.4426950408889634
LN2 = 0.6931471805599453
TILE = 256


def attention_kernel(n, scale, q_hbm, k_hbm, v_hbm, g_hbm, out_hbm, lse_hbm, dq_hbm, dk_hbm, dv_hbm,
                     k_all, v_all, turned, q_s, q_t, g_s, g_t, acc, run_m, run_l, delta, lse_s, out_s, dq_s, dk_s, dv_s,
                     dk_sum, dv_sum, dk_dn, dv_dn, dk_up, dv_up,
                     load_sem, swap_send, swap_recv, kv_up_send, kv_up_recv, kv_dn_send, kv_dn_recv,
                     dkv_dn_send, dkv_dn_recv, dkv_up_send, dkv_up_recv, store_sem, back_send, back_recv):
    heads, chunk, head_dim = q_s.shape
    half = chunk // 2
    tiles = chunk // TILE
    rank = lax.axis_index("cp")
    chip = rank // 2
    core = rank % 2
    other = 1 - core
    peer = 2 * chip + other
    above = 2 * ((chip + 1) % n) + core
    below = 2 * ((chip + n - 1) % n) + core
    mine = pl.ds(pl.multiple_of(core * half, half), half)
    theirs = pl.ds(pl.multiple_of(other * half, half), half)
    hops_up = (n // 2, n - 1 - n // 2)
    hops_dn = (n - 1 - n // 2, n // 2)
    kv_all = (k_all, v_all)
    sums = (dk_sum, dv_sum)
    from_up = (dk_dn, dv_dn)
    from_dn = (dk_up, dv_up)
    fold = scale * LOG2E

    def remote(src, dst, send_sem, recv_sem, device):
        return pltpu.make_async_remote_copy(src_ref=src, dst_ref=dst, send_sem=send_sem, recv_sem=recv_sem, device_id={"cp": device}, device_id_type=MESH)

    barrier = pltpu.get_barrier_semaphore()
    for device in (peer, above, below):
        pl.semaphore_signal(barrier, inc=1, device_id={"cp": device}, device_id_type=MESH)
    pl.semaphore_wait(barrier, 3)

    places = (k_all.at[chip, mine], v_all.at[chip, mine], q_s.at[:, mine], g_s.at[:, mine])
    sources = (k_hbm, v_hbm, q_hbm, g_hbm)
    swaps = [remote(sources[i].at[other], places[i], swap_send.at[i], swap_recv.at[i], peer) for i in range(4)]
    loads = [pltpu.make_async_copy(sources[i].at[core], places[i], load_sem.at[i]) for i in range(4)]
    for i in range(4):
        swaps[i].start()
        loads[i].start()

    def arrived(i):
        loads[i].wait()
        swaps[i].wait_recv()

    def kv_up(a, step, j):
        return remote(kv_all[a].at[j], kv_all[a].at[j], kv_up_send.at[a, step], kv_up_recv.at[a, step], above)

    def kv_dn(a, step, j):
        return remote(kv_all[a].at[j], kv_all[a].at[j], kv_dn_send.at[a, step], kv_dn_recv.at[a, step], below)

    def sends_up(a, step):
        return (chip < n - 1) & (chip - step >= 0) & (step < hops_up[a])

    def sends_dn(a, step):
        return ((chip + step) % n < hops_dn[a]) & (step < hops_dn[a])

    def own_up(a):
        @pl.when(sends_up(a, 0))
        def _():
            kv_up(a, 0, chip).start()

    def own_dn(a):
        @pl.when(sends_dn(a, 0))
        def _():
            kv_dn(a, 0, chip).start()

    arrived(0)
    own_up(0)
    own_dn(0)

    def take_up(a, step):
        j = chip - 1 - step

        @pl.when((j >= 0) & (step < hops_up[a]))
        def _():
            kv_up(a, step, j).wait_recv()

            @pl.when(sends_up(a, step + 1))
            def _():
                kv_up(a, step + 1, j).start()

    def take_dn(a, step):
        j = (chip + 1 + step) % n

        @pl.when((j < hops_dn[a]) & (step < hops_dn[a]))
        def _():
            kv_dn(a, step, j).wait_recv()

            @pl.when(sends_dn(a, step + 1))
            def _():
                kv_dn(a, step + 1, j).start()

    def turn(ref, j):
        for i in range(tiles):
            turned[:, i * TILE:(i + 1) * TILE] = ref[j, i * TILE:(i + 1) * TILE, :].T

    def causal(rows, i):
        key = lax.broadcasted_iota(jnp.int32, (rows, TILE), 0)
        query = lax.broadcasted_iota(jnp.int32, (rows, TILE), 1) + i * TILE
        return key <= query

    def scores(j, h, i, diagonal):
        cols = slice(i * TILE, (i + 1) * TILE)
        rows = (i + 1) * TILE if diagonal else chunk
        s = jnp.dot(k_all[j, :rows, :], q_t[h, :, cols], preferred_element_type=jnp.float32) * fold
        if diagonal:
            s = jnp.where(causal(rows, i), s, -jnp.inf)
        return cols, rows, s

    def stat_chunk(j, diagonal):
        def head(h, _):
            for i in range(tiles):
                cols, rows, s = scores(j, h, i, diagonal)
                top = jnp.max(s, axis=0, keepdims=True)
                if diagonal:
                    run_l[h, :, cols] = jnp.sum(jnp.exp2(s - top), axis=0, keepdims=True)
                else:
                    old = run_m[h, :, cols]
                    top = jnp.maximum(old, top)
                    run_l[h, :, cols] = run_l[h, :, cols] * jnp.exp2(old - top) + jnp.sum(jnp.exp2(s - top), axis=0, keepdims=True)
                run_m[h, :, cols] = top
            return 0

        lax.fori_loop(0, heads, head, 0)

    def value_chunk(j, diagonal, grad, output):
        if output:
            turn(v_all, j)
        if grad:
            dv_sum[j] = jnp.zeros((chunk, head_dim), jnp.float32)

        def head(h, _):
            for i in range(tiles):
                cols, rows, s = scores(j, h, i, diagonal)
                p = jnp.exp2(s - run_m[h, :, cols]).astype(jnp.bfloat16)
                if grad:
                    dv_sum[j, :rows, :] += jnp.dot(p, g_s[h, cols, :], preferred_element_type=jnp.float32)
                if output:
                    acc[h, :, cols] += jnp.dot(turned[:, :rows], p, preferred_element_type=jnp.float32)
            return 0

        lax.fori_loop(0, heads, head, 0)

    def key_chunk(j, diagonal):
        turn(k_all, j)
        dk_sum[j] = jnp.zeros((chunk, head_dim), jnp.float32)

        def head(h, _):
            for i in range(tiles):
                cols, rows, s = scores(j, h, i, diagonal)
                p = jnp.exp2(s - run_m[h, :, cols])
                dp = jnp.dot(v_all[j, :rows, :], g_t[h, :, cols], preferred_element_type=jnp.float32)
                ds = (p * (dp - delta[h, :, cols])).astype(jnp.bfloat16)
                dk_sum[j, :rows, :] += jnp.dot(ds, q_s[h, cols, :], preferred_element_type=jnp.float32)
                acc[h, :, cols] += jnp.dot(turned[:, :rows], ds, preferred_element_type=jnp.float32)
            return 0

        lax.fori_loop(0, heads, head, 0)

    arrived(2)

    def turn_q(h, _):
        for i in range(tiles):
            cols = slice(i * TILE, (i + 1) * TILE)
            q_t[h, :, cols] = q_s[h, cols, :].T
        return 0

    lax.fori_loop(0, heads, turn_q, 0)
    stat_chunk(chip, True)
    arrived(1)

    def stat_pos(s, _):
        step = s // 2
        up = s % 2 == 0

        @pl.when(up)
        def _():
            take_up(0, step)

            @pl.when(step == hops_up[0] - 1)
            def _():
                own_up(1)

        @pl.when(jnp.logical_not(up))
        def _():
            take_dn(0, step)

            @pl.when(step == hops_dn[0] - 1)
            def _():
                own_dn(1)

        j = jnp.where(up, chip - 1 - step, (chip + 1 + step) % n)
        valid = (j >= 0) & (j < chip) & (up | (j < hops_dn[0]))

        @pl.when(valid)
        def _():
            stat_chunk(j, False)

        return 0

    lax.fori_loop(0, n - 1, stat_pos, 0)

    arrived(3)

    def finish_stats(h, _):
        acc[h] = jnp.zeros((head_dim, chunk), jnp.float32)
        lse2 = run_m[h] + jnp.log2(run_l[h])
        run_m[h] = lse2
        lse_s[h] = lse2 * LN2
        for i in range(tiles):
            cols = slice(i * TILE, (i + 1) * TILE)
            g_t[h, :, cols] = g_s[h, cols, :].T
        return 0

    lax.fori_loop(0, heads, finish_stats, 0)

    def sum_dn(a, step, j):
        return remote(sums[a].at[j], from_up[a].at[step], dkv_dn_send.at[a, step], dkv_dn_recv.at[a, step], below)

    def sum_up(a, step, src):
        return remote(src, from_dn[a].at[step], dkv_up_send.at[a, step], dkv_up_recv.at[a, step], above)

    wide = n // 2

    def gives_dn(a, step):
        skip = (a == 0) & (step == 0) & (chip == n - 1)
        return (chip - hops_up[a] + step >= 0) & (step < hops_up[a]) & jnp.logical_not(skip)

    def gets_dn(a, step):
        skip = (a == 0) & (step == 1) & (chip == n - 2)
        return (step >= 1) & (chip < n - 1) & jnp.logical_not(skip)

    def up_index(step):
        return (chip + wide - step + n) % n

    def gives_up(a, step):
        j = up_index(step)
        return (j < wide) & (j != chip) & (step < wide) & ((a == 1) | (step >= 1) | (chip == n - 1))

    def gets_up(a, step):
        return (step >= 2 - a) | ((step >= 1) & (up_index(step) > chip))

    def add_in(a, j, part):
        sums[a][j] = sums[a][j] + part

    def pass_dn(a, step):
        @pl.when(gives_dn(a, step))
        def _():
            j = chip - hops_up[a] + step

            before = jnp.maximum(step - 1, 0)

            @pl.when(gets_dn(a, step))
            def _():
                sum_dn(a, before, j).wait_recv()
                add_in(a, j, from_up[a][before])

            sum_dn(a, step, j).start()

    def pass_up(a, step):
        @pl.when(gives_up(a, step))
        def _():
            j = up_index(step)
            before = jnp.maximum(step - 1, 0)

            @pl.when(gets_up(a, step))
            def _():
                sum_up(a, before, sums[a].at[j]).wait_recv()

            @pl.when(j < chip)
            def _():
                @pl.when(gets_up(a, step))
                def _():
                    add_in(a, j, from_dn[a][before])

                sum_up(a, step, sums[a].at[j]).start()

            @pl.when(j > chip)
            def _():
                sum_up(a, step, from_dn[a].at[before]).start()

    def place(s):
        step = jnp.maximum(s - 1, 0) // 2
        first = s == 0
        down = s % 2 == 1
        near = chip - hops_up[1] + step
        far = up_index(step + 1)
        j = jnp.where(first, chip - n // 2, jnp.where(down, near, far))
        valid = (j >= 0) & (j < chip) & (first | down | (j < wide))
        return step, first, down, j, valid

    early = 3

    def value_pos(s, _):
        step, first, down, j, valid = place(s)

        @pl.when(down)
        def _():
            take_up(1, step)
            take_dn(1, step)

        @pl.when(valid & (s < early))
        def _():
            value_chunk(j, False, True, False)

        @pl.when(valid & (s >= early))
        def _():
            value_chunk(j, False, True, True)

        @pl.when(first)
        def _():
            pass_up(1, 0)

        @pl.when(down)
        def _():
            pass_dn(1, step)

        @pl.when(jnp.logical_not(first | down))
        def _():
            pass_up(1, step + 1)

        @pl.when(s == early - 1)
        def _():
            value_chunk(chip, True, True, True)

        return 0

    lax.fori_loop(0, n - 1, value_pos, 0)
    take_dn(1, hops_dn[1] - 1)

    def output_pos(s, _):
        step, first, down, j, valid = place(early - 1 - s)

        @pl.when(valid)
        def _():
            value_chunk(j, False, False, True)

        return 0

    lax.fori_loop(0, early, output_pos, 0)

    def finish(h, _):
        for i in range(tiles):
            cols = slice(i * TILE, (i + 1) * TILE)
            out = acc[h, :, cols].astype(jnp.bfloat16)
            acc[h, :, cols] = jnp.zeros((head_dim, TILE), jnp.float32)
            delta[h, :, cols] = jnp.sum(g_t[h, :, cols].astype(jnp.float32) * out.astype(jnp.float32), axis=0, keepdims=True)
            out_s[h, cols, :] = out.T
        return 0

    lax.fori_loop(0, heads, finish, 0)

    def give_back(i, src_mine, src_theirs, dst):
        swap = remote(src_theirs, dst.at[core], back_send.at[i], back_recv.at[i], peer)
        keep = pltpu.make_async_copy(src_mine, dst.at[core], store_sem.at[i])
        swap.start()
        keep.start()
        return swap, keep

    pending = [
        give_back(0, out_s.at[:, mine], out_s.at[:, theirs], out_hbm),
        give_back(1, lse_s.at[:, :, mine], lse_s.at[:, :, theirs], lse_hbm),
    ]

    def key_pos(s, _):
        step, first, down, j, valid = place(s)

        @pl.when(valid)
        def _():
            key_chunk(j, False)

        @pl.when(first)
        def _():
            pass_dn(0, 0)
            pass_up(0, 0)

        @pl.when(down)
        def _():
            pass_dn(0, step + 1)

        @pl.when(jnp.logical_not(first | down))
        def _():
            pass_up(0, step + 1)

        @pl.when(s == n // 2 - 1)
        def _():
            key_chunk(chip, True)

        return 0

    lax.fori_loop(0, n - 1, key_pos, 0)

    def finish_q(h, _):
        for i in range(tiles):
            cols = slice(i * TILE, (i + 1) * TILE)
            dq_s[h, cols, :] = (acc[h, :, cols] * scale).astype(jnp.bfloat16).T
        return 0

    lax.fori_loop(0, heads, finish_q, 0)
    pending.append(give_back(2, dq_s.at[:, mine], dq_s.at[:, theirs], dq_hbm))

    for a in range(2):
        @pl.when(chip < wide)
        def _():
            sum_up(a, wide - 1, sums[a].at[chip]).wait_recv()
            add_in(a, chip, from_dn[a][wide - 1])

        @pl.when(chip < n - 1)
        def _():
            sum_dn(a, hops_up[a] - 1, chip).wait_recv()
            add_in(a, chip, from_up[a][hops_up[a] - 1])

        if a == 0:
            dk_s[...] = (dk_sum[chip] * scale).astype(jnp.bfloat16)
            pending.append(give_back(3, dk_s.at[mine], dk_s.at[theirs], dk_hbm))
        else:
            dv_s[...] = dv_sum[chip].astype(jnp.bfloat16)
            pending.append(give_back(4, dv_s.at[mine], dv_s.at[theirs], dv_hbm))

    for i in range(4):
        swaps[i].wait_send()
    for a in range(2):
        for step in range(hops_up[a]):
            @pl.when(sends_up(a, step))
            def _():
                kv_up(a, step, 0).wait_send()

            @pl.when(gives_dn(a, step))
            def _():
                sum_dn(a, step, 0).wait_send()

        for step in range(hops_dn[a]):
            @pl.when(sends_dn(a, step))
            def _():
                kv_dn(a, step, 0).wait_send()

        for step in range(wide):
            @pl.when(gives_up(a, step))
            def _():
                sum_up(a, step, sums[a].at[0]).wait_send()

    for swap, keep in pending:
        keep.wait()
        swap.wait()


def solution(mesh):
    chips = mesh.shape["cp"] // 2

    def attention_shard(queries, keys, values, out_grad):
        batch, tokens, heads, head_dim = queries.shape
        chunk = 2 * tokens
        half = chips // 2
        bf16, f32 = jnp.bfloat16, jnp.float32
        q = jnp.transpose(queries, (0, 2, 1, 3))
        g = jnp.transpose(out_grad, (0, 2, 1, 3))
        k = keys.reshape(batch, tokens, head_dim)
        v = values.reshape(batch, tokens, head_dim)
        any_spec = pl.BlockSpec(memory_space=pl.ANY)
        dma = pltpu.SemaphoreType.DMA
        out, lse, dq, dk, dv = pl.pallas_call(
            functools.partial(attention_kernel, chips, head_dim ** -0.5),
            out_shape=(
                jax.ShapeDtypeStruct(q.shape, bf16),
                jax.ShapeDtypeStruct((batch, heads, 1, tokens), f32),
                jax.ShapeDtypeStruct(q.shape, bf16),
                jax.ShapeDtypeStruct(k.shape, bf16),
                jax.ShapeDtypeStruct(k.shape, bf16),
            ),
            in_specs=[any_spec] * 4,
            out_specs=(any_spec,) * 5,
            scratch_shapes=[
                pltpu.VMEM((chips, chunk, head_dim), bf16),
                pltpu.VMEM((chips, chunk, head_dim), bf16),
                pltpu.VMEM((head_dim, chunk), bf16),
                pltpu.VMEM((heads, chunk, head_dim), bf16),
                pltpu.VMEM((heads, head_dim, chunk), bf16),
                pltpu.VMEM((heads, chunk, head_dim), bf16),
                pltpu.VMEM((heads, head_dim, chunk), bf16),
                pltpu.VMEM((heads, head_dim, chunk), f32),
                pltpu.VMEM((heads, 1, chunk), f32),
                pltpu.VMEM((heads, 1, chunk), f32),
                pltpu.VMEM((heads, 1, chunk), f32),
                pltpu.VMEM((heads, 1, chunk), f32),
                pltpu.VMEM((heads, chunk, head_dim), bf16),
                pltpu.VMEM((heads, chunk, head_dim), bf16),
                pltpu.VMEM((chunk, head_dim), bf16),
                pltpu.VMEM((chunk, head_dim), bf16),
                pltpu.VMEM((chips, chunk, head_dim), f32),
                pltpu.VMEM((chips, chunk, head_dim), f32),
                pltpu.VMEM((half, chunk, head_dim), f32),
                pltpu.VMEM((half - 1, chunk, head_dim), f32),
                pltpu.VMEM((half, chunk, head_dim), f32),
                pltpu.VMEM((half, chunk, head_dim), f32),
                dma((4,)), dma((4,)), dma((4,)),
                dma((2, half)), dma((2, half)), dma((2, half)), dma((2, half)),
                dma((2, half)), dma((2, half)), dma((2, half)), dma((2, half)),
                dma((5,)), dma((5,)), dma((5,)),
            ],
            compiler_params=pltpu.CompilerParams(collective_id=0, has_side_effects=True, vmem_limit_bytes=67043328),
            name="ring_attention",
        )(q, k, v, g)
        back = (0, 2, 1, 3)
        return (
            jnp.transpose(out, back),
            lse.reshape(batch, heads, tokens),
            jnp.transpose(dq, back),
            dk.reshape(keys.shape),
            dv.reshape(values.shape),
        )

    seq_spec = P("dp", "cp")
    return jax.shard_map(attention_shard, mesh=mesh, in_specs=(seq_spec,) * 4, out_specs=(seq_spec, P("dp", None, "cp"), seq_spec, seq_spec, seq_spec), check_vma=False)
```

```python
import functools

import jax
import jax.numpy as jnp
from jax import lax
from jax.experimental import pallas as pl
from jax.experimental.pallas import tpu as pltpu
from jax.sharding import PartitionSpec as P

MESH = pl.DeviceIdType.MESH
LOG2E = 1.4426950408889634
LN2 = 0.6931471805599453
TILE = 256
GO_AT = 3


def attention_kernel(n, scale, q_hbm, k_hbm, v_hbm, g_hbm, out_hbm, lse_hbm, dq_hbm, dk_hbm, dv_hbm,
                     k_all, v_all, turned, q_s, q_t, g_s, g_t, acc, run_m, run_l, delta, lse_s, out_s, dq_s, dk_s, dv_s,
                     dk_sum, dv_sum, dk_dn, dv_dn, dk_up, dv_up,
                     load_sem, swap_send, swap_recv, kv_up_send, kv_up_recv, kv_dn_send, kv_dn_recv,
                     dkv_dn_send, dkv_dn_recv, dkv_up_send, dkv_up_recv, store_sem, back_send, back_recv, go_sem):
    heads, chunk, head_dim = q_s.shape
    half = chunk // 2
    tiles = chunk // TILE
    rank = lax.axis_index("cp")
    chip = rank // 2
    core = rank % 2
    other = 1 - core
    peer = 2 * chip + other
    above = 2 * ((chip + 1) % n) + core
    below = 2 * ((chip + n - 1) % n) + core
    mine = pl.ds(pl.multiple_of(core * half, half), half)
    theirs = pl.ds(pl.multiple_of(other * half, half), half)
    hops_up = (n // 2, n - 1 - n // 2)
    hops_dn = (n - 1 - n // 2, n // 2)
    kv_all = (k_all, v_all)
    sums = (dk_sum, dv_sum)
    from_up = (dk_dn, dv_dn)
    from_dn = (dk_up, dv_up)
    fold = scale * LOG2E

    def remote(src, dst, send_sem, recv_sem, device):
        return pltpu.make_async_remote_copy(src_ref=src, dst_ref=dst, send_sem=send_sem, recv_sem=recv_sem, device_id={"cp": device}, device_id_type=MESH)

    barrier = pltpu.get_barrier_semaphore()
    for device in (peer, above, below):
        pl.semaphore_signal(barrier, inc=1, device_id={"cp": device}, device_id_type=MESH)
    pl.semaphore_wait(barrier, 3)

    places = (k_all.at[chip, mine], v_all.at[chip, mine], q_s.at[:, mine], g_s.at[:, mine])
    sources = (k_hbm, v_hbm, q_hbm, g_hbm)
    swaps = [remote(sources[i].at[other], places[i], swap_send.at[i], swap_recv.at[i], peer) for i in range(4)]
    loads = [pltpu.make_async_copy(sources[i].at[core], places[i], load_sem.at[i]) for i in range(4)]
    for i in range(4):
        swaps[i].start()
        loads[i].start()

    def arrived(i):
        loads[i].wait()
        swaps[i].wait_recv()

    def kv_up(a, step, j):
        return remote(kv_all[a].at[j], kv_all[a].at[j], kv_up_send.at[a, step], kv_up_recv.at[a, step], above)

    def kv_dn(a, step, j):
        return remote(kv_all[a].at[j], kv_all[a].at[j], kv_dn_send.at[a, step], kv_dn_recv.at[a, step], below)

    def sends_up(a, step):
        return (chip < n - 1) & (chip - step >= 0) & (step < hops_up[a])

    def sends_dn(a, step):
        return ((chip + step) % n < hops_dn[a]) & (step < hops_dn[a])

    def send_own(a):
        @pl.when(sends_up(a, 0))
        def _():
            kv_up(a, 0, chip).start()

        @pl.when(sends_dn(a, 0))
        def _():
            kv_dn(a, 0, chip).start()

    for a in range(2):
        arrived(a)

        @pl.when(core == 0)
        def _():
            send_own(a)

    def take_up(a, step):
        j = chip - 1 - step

        @pl.when((j >= 0) & (step < hops_up[a]))
        def _():
            kv_up(a, step, j).wait_recv()

            @pl.when(sends_up(a, step + 1))
            def _():
                kv_up(a, step + 1, j).start()

    def take_dn(a, step):
        j = (chip + 1 + step) % n

        @pl.when((j < hops_dn[a]) & (step < hops_dn[a]))
        def _():
            kv_dn(a, step, j).wait_recv()

            @pl.when(sends_dn(a, step + 1))
            def _():
                kv_dn(a, step + 1, j).start()

    def turn(ref, j):
        for i in range(tiles):
            turned[:, i * TILE:(i + 1) * TILE] = ref[j, i * TILE:(i + 1) * TILE, :].T

    def causal(rows, i):
        key = lax.broadcasted_iota(jnp.int32, (rows, TILE), 0)
        query = lax.broadcasted_iota(jnp.int32, (rows, TILE), 1) + i * TILE
        return key <= query

    def forward_chunk(j, diagonal):
        turn(v_all, j)

        def head(h, _):
            for i in range(tiles):
                cols = slice(i * TILE, (i + 1) * TILE)
                rows = (i + 1) * TILE if diagonal else chunk
                s = jnp.dot(k_all[j, :rows, :], q_t[h, :, cols], preferred_element_type=jnp.float32) * fold
                if diagonal:
                    s = jnp.where(causal(rows, i), s, -jnp.inf)
                    top = jnp.max(s, axis=0, keepdims=True)
                else:
                    old = run_m[h, :, cols]
                    top = jnp.maximum(old, jnp.max(s, axis=0, keepdims=True))
                p = jnp.exp2(s - top)
                total = jnp.sum(p, axis=0, keepdims=True)
                part = jnp.dot(turned[:, :rows], p.astype(jnp.bfloat16), preferred_element_type=jnp.float32)
                run_m[h, :, cols] = top
                if diagonal:
                    run_l[h, :, cols] = total
                    acc[h, :, cols] = part
                else:
                    alpha = jnp.exp2(old - top)
                    run_l[h, :, cols] = run_l[h, :, cols] * alpha + total
                    acc[h, :, cols] = acc[h, :, cols] * alpha + part
            return 0

        lax.fori_loop(0, heads, head, 0, unroll=True)

    arrived(2)

    def turn_q(h, _):
        for i in range(tiles):
            cols = slice(i * TILE, (i + 1) * TILE)
            q_t[h, :, cols] = q_s[h, cols, :].T
        return 0

    lax.fori_loop(0, heads, turn_q, 0)
    forward_chunk(chip, True)
    arrived(3)

    def turn_g(h, _):
        for i in range(tiles):
            cols = slice(i * TILE, (i + 1) * TILE)
            g_t[h, :, cols] = g_s[h, cols, :].T
        return 0

    lax.fori_loop(0, heads, turn_g, 0)

    @pl.when(core == 1)
    def _():
        pl.semaphore_wait(go_sem, 1)
        send_own(0)
        send_own(1)

    def forward_pos(s, _):
        step = s // 2
        up = s % 2 == 0
        last = s == n - 2

        @pl.when(up)
        def _():
            take_up(0, step)
            take_up(1, step)

        @pl.when(jnp.logical_not(up))
        def _():
            take_dn(0, step)
            take_dn(1, step)

        @pl.when(last)
        def _():
            take_dn(1, step)

        @pl.when((core == 0) & (s == GO_AT))
        def _():
            pl.semaphore_signal(go_sem, inc=1, device_id={"cp": peer}, device_id_type=MESH)

        j = jnp.where(up, chip - 1 - step, (chip + 1 + step) % n)
        valid = (j >= 0) & (j < chip) & (up | (j < hops_dn[0]))

        @pl.when(valid)
        def _():
            forward_chunk(j, False)

        return 0

    lax.fori_loop(0, n - 1, forward_pos, 0)

    def finish(h, _):
        for i in range(tiles):
            cols = slice(i * TILE, (i + 1) * TILE)
            total = run_l[h, :, cols]
            out = (acc[h, :, cols] / total).astype(jnp.bfloat16)
            acc[h, :, cols] = jnp.zeros((head_dim, TILE), jnp.float32)
            delta[h, :, cols] = jnp.sum(g_t[h, :, cols].astype(jnp.float32) * out.astype(jnp.float32), axis=0, keepdims=True)
            lse2 = run_m[h, :, cols] + jnp.log2(total)
            run_m[h, :, cols] = lse2
            lse_s[h, :, cols] = lse2 * LN2
            out_s[h, cols, :] = out.T
        return 0

    lax.fori_loop(0, heads, finish, 0)

    def give_back(i, src_mine, src_theirs, dst):
        swap = remote(src_theirs, dst.at[core], back_send.at[i], back_recv.at[i], peer)
        keep = pltpu.make_async_copy(src_mine, dst.at[core], store_sem.at[i])
        swap.start()
        keep.start()
        return swap, keep

    pending = [
        give_back(0, out_s.at[:, mine], out_s.at[:, theirs], out_hbm),
        give_back(1, lse_s.at[:, :, mine], lse_s.at[:, :, theirs], lse_hbm),
    ]

    def backward_chunk(j, diagonal):
        turn(k_all, j)
        dk_sum[j] = jnp.zeros((chunk, head_dim), jnp.float32)
        dv_sum[j] = jnp.zeros((chunk, head_dim), jnp.float32)

        def head(h, _):
            size = [(i + 1) * TILE if diagonal else chunk for i in range(tiles)]
            cols = [slice(i * TILE, (i + 1) * TILE) for i in range(tiles)]
            ps, dss = [], []
            for i in range(tiles):
                s = jnp.dot(k_all[j, :size[i], :], q_t[h, :, cols[i]], preferred_element_type=jnp.float32)
                dp = jnp.dot(v_all[j, :size[i], :], g_t[h, :, cols[i]], preferred_element_type=jnp.float32)
                if diagonal:
                    s = jnp.where(causal(size[i], i), s, -jnp.inf)
                p = jnp.exp2(s * fold - run_m[h, :, cols[i]])
                ps.append(p.astype(jnp.bfloat16))
                dss.append((p * (dp - delta[h, :, cols[i]])).astype(jnp.bfloat16))
            if diagonal:
                for i in range(tiles):
                    dv_sum[j, :size[i], :] += jnp.dot(ps[i], g_s[h, cols[i], :], preferred_element_type=jnp.float32)
                    dk_sum[j, :size[i], :] += jnp.dot(dss[i], q_s[h, cols[i], :], preferred_element_type=jnp.float32)
                    acc[h, :, cols[i]] += jnp.dot(turned[:, :size[i]], dss[i], preferred_element_type=jnp.float32)
            else:
                pp = jnp.concatenate(ps, axis=1)
                dd = jnp.concatenate(dss, axis=1)
                dv_sum[j] += jnp.dot(pp, g_s[h], preferred_element_type=jnp.float32)
                dk_sum[j] += jnp.dot(dd, q_s[h], preferred_element_type=jnp.float32)
                acc[h] += jnp.dot(turned[...], dd, preferred_element_type=jnp.float32)
            return 0

        lax.fori_loop(0, heads, head, 0, unroll=2)

    def sum_dn(a, step, j):
        return remote(sums[a].at[j], from_up[a].at[step], dkv_dn_send.at[a, step], dkv_dn_recv.at[a, step], below)

    def sum_up(a, step, src):
        return remote(src, from_dn[a].at[step], dkv_up_send.at[a, step], dkv_up_recv.at[a, step], above)

    wide = n // 2
    wrap = False

    def gives_dn(a, step):
        skip = (a == 0) & (step == 0) & (chip == n - 1) & wrap
        return (chip - hops_up[a] + step >= 0) & (step < hops_up[a]) & jnp.logical_not(skip)

    def gets_dn(a, step):
        skip = (a == 0) & (step == 1) & (chip == n - 2) & wrap
        return (step >= 1) & (chip < n - 1) & jnp.logical_not(skip)

    def up_index(step):
        return (chip + wide - step + n) % n

    def gives_up(a, step):
        j = up_index(step)
        in_reach = (j < wide) & (j != chip) & (step < wide)
        if a == 0:
            in_reach &= (wrap & (chip == n - 1)) | ((step >= 1) & (wrap | (j < wide - 1)))
        return in_reach

    def gets_up(a, step):
        return (step >= 2 - a) | ((step >= 1) & (up_index(step) > chip))

    def add_in(a, j, part):
        sums[a][j] = sums[a][j] + part

    def pass_dn(a, step):
        @pl.when(gives_dn(a, step))
        def _():
            j = chip - hops_up[a] + step

            before = jnp.maximum(step - 1, 0)

            @pl.when(gets_dn(a, step))
            def _():
                sum_dn(a, before, j).wait_recv()
                add_in(a, j, from_up[a][before])

            sum_dn(a, step, j).start()

    def pass_up(a, step):
        @pl.when(gives_up(a, step))
        def _():
            j = up_index(step)
            before = jnp.maximum(step - 1, 0)

            @pl.when(gets_up(a, step))
            def _():
                sum_up(a, before, sums[a].at[j]).wait_recv()

            @pl.when(j < chip)
            def _():
                @pl.when(gets_up(a, step))
                def _():
                    add_in(a, j, from_dn[a][before])

                sum_up(a, step, sums[a].at[j]).start()

            @pl.when(j > chip)
            def _():
                sum_up(a, step, from_dn[a].at[before]).start()

    def backward_pos(s, _):
        step = jnp.maximum(s - 1, 0) // 2
        first = s == 0
        down = s % 2 == 1
        near = chip - hops_up[1] + step
        far = up_index(step + 1)
        j = jnp.where(first, chip - n // 2, jnp.where(down, near, far))
        valid = (j >= 0) & (j < chip) & (first | down | (j < wide))

        @pl.when(valid)
        def _():
            backward_chunk(j, False)

        @pl.when(first)
        def _():
            pass_dn(0, 0)
            pass_up(0, 0)
            pass_up(1, 0)

        @pl.when(down)
        def _():
            pass_dn(0, step + 1)
            pass_dn(1, step)

        @pl.when(jnp.logical_not(first | down))
        def _():
            pass_up(0, step + 1)
            pass_up(1, step + 1)

        @pl.when(s == n // 2 - 1)
        def _():
            backward_chunk(chip, True)

        return 0

    lax.fori_loop(0, n - 1, backward_pos, 0)

    def finish_q(h, _):
        for i in range(tiles):
            cols = slice(i * TILE, (i + 1) * TILE)
            dq_s[h, cols, :] = (acc[h, :, cols] * scale).astype(jnp.bfloat16).T
        return 0

    lax.fori_loop(0, heads, finish_q, 0)
    pending.append(give_back(2, dq_s.at[:, mine], dq_s.at[:, theirs], dq_hbm))

    for a in range(2):
        @pl.when((chip < wide) if a == 1 else (chip < wide - 1) | (wrap & (chip < wide)))
        def _():
            sum_up(a, wide - 1, sums[a].at[chip]).wait_recv()
            add_in(a, chip, from_dn[a][wide - 1])

        @pl.when(chip < n - 1)
        def _():
            sum_dn(a, hops_up[a] - 1, chip).wait_recv()
            add_in(a, chip, from_up[a][hops_up[a] - 1])

        if a == 0:
            dk_s[...] = (dk_sum[chip] * scale).astype(jnp.bfloat16)
            pending.append(give_back(3, dk_s.at[mine], dk_s.at[theirs], dk_hbm))
        else:
            dv_s[...] = dv_sum[chip].astype(jnp.bfloat16)
            pending.append(give_back(4, dv_s.at[mine], dv_s.at[theirs], dv_hbm))

    for i in range(4):
        swaps[i].wait_send()
    for a in range(2):
        for step in range(hops_up[a]):
            @pl.when(sends_up(a, step))
            def _():
                kv_up(a, step, 0).wait_send()

            @pl.when(gives_dn(a, step))
            def _():
                sum_dn(a, step, 0).wait_send()

        for step in range(hops_dn[a]):
            @pl.when(sends_dn(a, step))
            def _():
                kv_dn(a, step, 0).wait_send()

        for step in range(wide):
            @pl.when(gives_up(a, step))
            def _():
                sum_up(a, step, sums[a].at[0]).wait_send()

    for swap, keep in pending:
        keep.wait()
        swap.wait()


def solution(mesh):
    chips = mesh.shape["cp"] // 2

    def attention_shard(queries, keys, values, out_grad):
        batch, tokens, heads, head_dim = queries.shape
        chunk = 2 * tokens
        half = chips // 2
        bf16, f32 = jnp.bfloat16, jnp.float32
        q = jnp.transpose(queries, (0, 2, 1, 3))
        g = jnp.transpose(out_grad, (0, 2, 1, 3))
        k = keys.reshape(batch, tokens, head_dim)
        v = values.reshape(batch, tokens, head_dim)
        any_spec = pl.BlockSpec(memory_space=pl.ANY)
        dma = pltpu.SemaphoreType.DMA
        out, lse, dq, dk, dv = pl.pallas_call(
            functools.partial(attention_kernel, chips, head_dim ** -0.5),
            out_shape=(
                jax.ShapeDtypeStruct(q.shape, bf16),
                jax.ShapeDtypeStruct((batch, heads, 1, tokens), f32),
                jax.ShapeDtypeStruct(q.shape, bf16),
                jax.ShapeDtypeStruct(k.shape, bf16),
                jax.ShapeDtypeStruct(k.shape, bf16),
            ),
            in_specs=[any_spec] * 4,
            out_specs=(any_spec,) * 5,
            scratch_shapes=[
                pltpu.VMEM((chips, chunk, head_dim), bf16),
                pltpu.VMEM((chips, chunk, head_dim), bf16),
                pltpu.VMEM((head_dim, chunk), bf16),
                pltpu.VMEM((heads, chunk, head_dim), bf16),
                pltpu.VMEM((heads, head_dim, chunk), bf16),
                pltpu.VMEM((heads, chunk, head_dim), bf16),
                pltpu.VMEM((heads, head_dim, chunk), bf16),
                pltpu.VMEM((heads, head_dim, chunk), f32),
                pltpu.VMEM((heads, 1, chunk), f32),
                pltpu.VMEM((heads, 1, chunk), f32),
                pltpu.VMEM((heads, 1, chunk), f32),
                pltpu.VMEM((heads, 1, chunk), f32),
                pltpu.VMEM((heads, chunk, head_dim), bf16),
                pltpu.VMEM((heads, chunk, head_dim), bf16),
                pltpu.VMEM((chunk, head_dim), bf16),
                pltpu.VMEM((chunk, head_dim), bf16),
                pltpu.VMEM((chips, chunk, head_dim), f32),
                pltpu.VMEM((chips, chunk, head_dim), f32),
                pltpu.VMEM((half, chunk, head_dim), f32),
                pltpu.VMEM((half - 1, chunk, head_dim), f32),
                pltpu.VMEM((half, chunk, head_dim), f32),
                pltpu.VMEM((half, chunk, head_dim), f32),
                dma((4,)), dma((4,)), dma((4,)),
                dma((2, half)), dma((2, half)), dma((2, half)), dma((2, half)),
                dma((2, half)), dma((2, half)), dma((2, half)), dma((2, half)),
                dma((5,)), dma((5,)), dma((5,)), pltpu.SemaphoreType.REGULAR,
            ],
            compiler_params=pltpu.CompilerParams(collective_id=0, has_side_effects=True, vmem_limit_bytes=67043328),
            name="ring_attention",
        )(q, k, v, g)
        back = (0, 2, 1, 3)
        return (
            jnp.transpose(out, back),
            lse.reshape(batch, heads, tokens),
            jnp.transpose(dq, back),
            dk.reshape(keys.shape),
            dv.reshape(values.shape),
        )

    seq_spec = P("dp", "cp")
    return jax.shard_map(attention_shard, mesh=mesh, in_specs=(seq_spec,) * 4, out_specs=(seq_spec, P("dp", None, "cp"), seq_spec, seq_spec, seq_spec), check_vma=False)
```

```python
import functools

import jax
import jax.numpy as jnp
from jax import lax
from jax.experimental import pallas as pl
from jax.experimental.pallas import tpu as pltpu
from jax.sharding import PartitionSpec as P

MESH = pl.DeviceIdType.MESH
LOG2E = 1.4426950408889634
LN2 = 0.6931471805599453
TILE = 256
GO_AT = 1


def attention_kernel(n, scale, q_hbm, k_hbm, v_hbm, g_hbm, out_hbm, lse_hbm, dq_hbm, dk_hbm, dv_hbm,
                     k_all, v_all, turned, q_s, q_t, g_s, g_t, acc, run_m, run_l, delta, lse_s, out_s, dq_s, dk_s, dv_s,
                     dk_sum, dv_sum, dk_dn, dv_dn, dk_up, dv_up,
                     load_sem, swap_send, swap_recv, kv_up_send, kv_up_recv, kv_dn_send, kv_dn_recv,
                     dkv_dn_send, dkv_dn_recv, dkv_up_send, dkv_up_recv, store_sem, back_send, back_recv, go_sem):
    heads, chunk, head_dim = q_s.shape
    half = chunk // 2
    tiles = chunk // TILE
    rank = lax.axis_index("cp")
    chip = rank // 2
    core = rank % 2
    other = 1 - core
    peer = 2 * chip + other
    above = 2 * ((chip + 1) % n) + core
    below = 2 * ((chip + n - 1) % n) + core
    mine = pl.ds(pl.multiple_of(core * half, half), half)
    theirs = pl.ds(pl.multiple_of(other * half, half), half)
    hops_up = (n // 2, n - 1 - n // 2)
    hops_dn = (n - 1 - n // 2, n // 2)
    kv_all = (k_all, v_all)
    sums = (dk_sum, dv_sum)
    from_up = (dk_dn, dv_dn)
    from_dn = (dk_up, dv_up)
    fold = scale * LOG2E

    def remote(src, dst, send_sem, recv_sem, device):
        return pltpu.make_async_remote_copy(src_ref=src, dst_ref=dst, send_sem=send_sem, recv_sem=recv_sem, device_id={"cp": device}, device_id_type=MESH)

    barrier = pltpu.get_barrier_semaphore()
    for device in (peer, above, below):
        pl.semaphore_signal(barrier, inc=1, device_id={"cp": device}, device_id_type=MESH)
    pl.semaphore_wait(barrier, 3)

    places = (k_all.at[chip, mine], v_all.at[chip, mine], q_s.at[:, mine], g_s.at[:, mine])
    sources = (k_hbm, v_hbm, q_hbm, g_hbm)
    swaps = [remote(sources[i].at[other], places[i], swap_send.at[i], swap_recv.at[i], peer) for i in range(4)]
    loads = [pltpu.make_async_copy(sources[i].at[core], places[i], load_sem.at[i]) for i in range(4)]
    for i in range(4):
        swaps[i].start()
        loads[i].start()

    def arrived(i):
        loads[i].wait()
        swaps[i].wait_recv()

    def kv_up(a, step, j):
        return remote(kv_all[a].at[j], kv_all[a].at[j], kv_up_send.at[a, step], kv_up_recv.at[a, step], above)

    def kv_dn(a, step, j):
        return remote(kv_all[a].at[j], kv_all[a].at[j], kv_dn_send.at[a, step], kv_dn_recv.at[a, step], below)

    def sends_up(a, step):
        return (chip < n - 1) & (chip - step >= 0) & (step < hops_up[a])

    def sends_dn(a, step):
        return ((chip + step) % n < hops_dn[a]) & (step < hops_dn[a])

    def send_own(a):
        @pl.when(sends_up(a, 0))
        def _():
            kv_up(a, 0, chip).start()

        @pl.when(sends_dn(a, 0))
        def _():
            kv_dn(a, 0, chip).start()

    for a in range(2):
        arrived(a)

        @pl.when(core == 0)
        def _():
            send_own(a)

    def take_up(a, step):
        j = chip - 1 - step

        @pl.when((j >= 0) & (step < hops_up[a]))
        def _():
            kv_up(a, step, j).wait_recv()

            @pl.when(sends_up(a, step + 1))
            def _():
                kv_up(a, step + 1, j).start()

    def take_dn(a, step):
        j = (chip + 1 + step) % n

        @pl.when((j < hops_dn[a]) & (step < hops_dn[a]))
        def _():
            kv_dn(a, step, j).wait_recv()

            @pl.when(sends_dn(a, step + 1))
            def _():
                kv_dn(a, step + 1, j).start()

    def turn(ref, j):
        for i in range(tiles):
            turned[:, i * TILE:(i + 1) * TILE] = ref[j, i * TILE:(i + 1) * TILE, :].T

    def causal(rows, i):
        key = lax.broadcasted_iota(jnp.int32, (rows, TILE), 0)
        query = lax.broadcasted_iota(jnp.int32, (rows, TILE), 1) + i * TILE
        return key <= query

    def forward_chunk(j, diagonal):
        turn(v_all, j)

        def head(h, _):
            for i in range(tiles):
                cols = slice(i * TILE, (i + 1) * TILE)
                rows = (i + 1) * TILE if diagonal else chunk
                s = jnp.dot(k_all[j, :rows, :], q_t[h, :, cols], preferred_element_type=jnp.float32) * fold
                if diagonal:
                    s = jnp.where(causal(rows, i), s, -jnp.inf)
                    top = jnp.max(s, axis=0, keepdims=True)
                else:
                    old = run_m[h, :, cols]
                    top = jnp.maximum(old, jnp.max(s, axis=0, keepdims=True))
                p = jnp.exp2(s - top)
                total = jnp.sum(p, axis=0, keepdims=True)
                part = jnp.dot(turned[:, :rows], p.astype(jnp.bfloat16), preferred_element_type=jnp.float32)
                run_m[h, :, cols] = top
                if diagonal:
                    run_l[h, :, cols] = total
                    acc[h, :, cols] = part
                else:
                    alpha = jnp.exp2(old - top)
                    run_l[h, :, cols] = run_l[h, :, cols] * alpha + total
                    acc[h, :, cols] = acc[h, :, cols] * alpha + part
            return 0

        lax.fori_loop(0, heads, head, 0, unroll=True)

    arrived(2)

    def turn_q(h, _):
        for i in range(tiles):
            cols = slice(i * TILE, (i + 1) * TILE)
            q_t[h, :, cols] = q_s[h, cols, :].T
        return 0

    lax.fori_loop(0, heads, turn_q, 0)
    forward_chunk(chip, True)
    arrived(3)

    def turn_g(h, _):
        for i in range(tiles):
            cols = slice(i * TILE, (i + 1) * TILE)
            g_t[h, :, cols] = g_s[h, cols, :].T
        return 0

    lax.fori_loop(0, heads, turn_g, 0)

    @pl.when(core == 1)
    def _():
        pl.semaphore_wait(go_sem, 1)
        send_own(0)
        send_own(1)

    def forward_step(step, _):
        for a in range(2):
            take_up(a, step)
            take_dn(a, step)

        @pl.when((core == 0) & (step == GO_AT))
        def _():
            pl.semaphore_signal(go_sem, inc=1, device_id={"cp": peer}, device_id_type=MESH)

        def use(side, _):
            j = jnp.where(side == 0, chip - 1 - step, (chip + 1 + step) % n)
            valid = (j >= 0) & (j < chip) & ((side == 0) | ((j < hops_dn[0]) & (step < hops_dn[0])))

            @pl.when(valid)
            def _():
                forward_chunk(j, False)

            return 0

        lax.fori_loop(0, 2, use, 0)
        return 0

    lax.fori_loop(0, n // 2, forward_step, 0)

    def finish(h, _):
        for i in range(tiles):
            cols = slice(i * TILE, (i + 1) * TILE)
            total = run_l[h, :, cols]
            out = (acc[h, :, cols] / total).astype(jnp.bfloat16)
            acc[h, :, cols] = jnp.zeros((head_dim, TILE), jnp.float32)
            delta[h, :, cols] = jnp.sum(g_t[h, :, cols].astype(jnp.float32) * out.astype(jnp.float32), axis=0, keepdims=True)
            lse2 = run_m[h, :, cols] + jnp.log2(total)
            run_m[h, :, cols] = lse2
            lse_s[h, :, cols] = lse2 * LN2
            out_s[h, cols, :] = out.T
        return 0

    lax.fori_loop(0, heads, finish, 0)

    def give_back(i, src_mine, src_theirs, dst):
        swap = remote(src_theirs, dst.at[core], back_send.at[i], back_recv.at[i], peer)
        keep = pltpu.make_async_copy(src_mine, dst.at[core], store_sem.at[i])
        swap.start()
        keep.start()
        return swap, keep

    pending = [
        give_back(0, out_s.at[:, mine], out_s.at[:, theirs], out_hbm),
        give_back(1, lse_s.at[:, :, mine], lse_s.at[:, :, theirs], lse_hbm),
    ]

    def backward_chunk(j, diagonal):
        turn(k_all, j)
        dk_sum[j] = jnp.zeros((chunk, head_dim), jnp.float32)
        dv_sum[j] = jnp.zeros((chunk, head_dim), jnp.float32)

        def head(h, _):
            size = [(i + 1) * TILE if diagonal else chunk for i in range(tiles)]
            cols = [slice(i * TILE, (i + 1) * TILE) for i in range(tiles)]
            ps, dss = [], []
            for i in range(tiles):
                s = jnp.dot(k_all[j, :size[i], :], q_t[h, :, cols[i]], preferred_element_type=jnp.float32)
                dp = jnp.dot(v_all[j, :size[i], :], g_t[h, :, cols[i]], preferred_element_type=jnp.float32)
                if diagonal:
                    s = jnp.where(causal(size[i], i), s, -jnp.inf)
                p = jnp.exp2(s * fold - run_m[h, :, cols[i]])
                ps.append(p.astype(jnp.bfloat16))
                dss.append((p * (dp - delta[h, :, cols[i]])).astype(jnp.bfloat16))
            if diagonal:
                for i in range(tiles):
                    dv_sum[j, :size[i], :] += jnp.dot(ps[i], g_s[h, cols[i], :], preferred_element_type=jnp.float32)
                    dk_sum[j, :size[i], :] += jnp.dot(dss[i], q_s[h, cols[i], :], preferred_element_type=jnp.float32)
                    acc[h, :, cols[i]] += jnp.dot(turned[:, :size[i]], dss[i], preferred_element_type=jnp.float32)
            else:
                pp = jnp.concatenate(ps, axis=1)
                dd = jnp.concatenate(dss, axis=1)
                dv_sum[j] += jnp.dot(pp, g_s[h], preferred_element_type=jnp.float32)
                dk_sum[j] += jnp.dot(dd, q_s[h], preferred_element_type=jnp.float32)
                acc[h] += jnp.dot(turned[...], dd, preferred_element_type=jnp.float32)
            return 0

        lax.fori_loop(0, heads, head, 0, unroll=2)

    def sum_dn(a, step, j):
        return remote(sums[a].at[j], from_up[a].at[step], dkv_dn_send.at[a, step], dkv_dn_recv.at[a, step], below)

    def sum_up(a, step, src):
        return remote(src, from_dn[a].at[step], dkv_up_send.at[a, step], dkv_up_recv.at[a, step], above)

    wide = n // 2
    wrap = False

    def gives_dn(a, step):
        skip = (a == 0) & (step == 0) & (chip == n - 1) & wrap
        return (chip - hops_up[a] + step >= 0) & (step < hops_up[a]) & jnp.logical_not(skip)

    def gets_dn(a, step):
        skip = (a == 0) & (step == 1) & (chip == n - 2) & wrap
        return (step >= 1) & (chip < n - 1) & jnp.logical_not(skip)

    def up_index(step):
        return (chip + wide - step + n) % n

    def gives_up(a, step):
        j = up_index(step)
        in_reach = (j < wide) & (j != chip) & (step < wide)
        if a == 0:
            in_reach &= (wrap & (chip == n - 1)) | ((step >= 1) & (wrap | (j < wide - 1)))
        return in_reach

    def gets_up(a, step):
        return (step >= 2 - a) | ((step >= 1) & (up_index(step) > chip))

    def add_in(a, j, part):
        sums[a][j] = sums[a][j] + part

    def pass_dn(a, step):
        @pl.when(gives_dn(a, step))
        def _():
            j = chip - hops_up[a] + step

            before = jnp.maximum(step - 1, 0)

            @pl.when(gets_dn(a, step))
            def _():
                sum_dn(a, before, j).wait_recv()
                add_in(a, j, from_up[a][before])

            sum_dn(a, step, j).start()

    def pass_up(a, step):
        @pl.when(gives_up(a, step))
        def _():
            j = up_index(step)
            before = jnp.maximum(step - 1, 0)

            @pl.when(gets_up(a, step))
            def _():
                sum_up(a, before, sums[a].at[j]).wait_recv()

            @pl.when(j < chip)
            def _():
                @pl.when(gets_up(a, step))
                def _():
                    add_in(a, j, from_dn[a][before])

                sum_up(a, step, sums[a].at[j]).start()

            @pl.when(j > chip)
            def _():
                sum_up(a, step, from_dn[a].at[before]).start()

    def backward_pos(s, _):
        step = jnp.maximum(s - 1, 0) // 2
        first = s == 0
        down = s % 2 == 1
        near = chip - hops_up[1] + step
        far = up_index(step + 1)
        j = jnp.where(first, chip - n // 2, jnp.where(down, near, far))
        valid = (j >= 0) & (j < chip) & (first | down | (j < wide))

        @pl.when(valid)
        def _():
            backward_chunk(j, False)

        @pl.when(first)
        def _():
            pass_dn(0, 0)
            pass_up(0, 0)
            pass_up(1, 0)

        @pl.when(down)
        def _():
            pass_dn(0, step + 1)
            pass_dn(1, step)

        @pl.when(jnp.logical_not(first | down))
        def _():
            pass_up(0, step + 1)
            pass_up(1, step + 1)

        @pl.when(s == n // 2 - 1)
        def _():
            backward_chunk(chip, True)

        return 0

    lax.fori_loop(0, n - 1, backward_pos, 0)

    def finish_q(h, _):
        for i in range(tiles):
            cols = slice(i * TILE, (i + 1) * TILE)
            dq_s[h, cols, :] = (acc[h, :, cols] * scale).astype(jnp.bfloat16).T
        return 0

    lax.fori_loop(0, heads, finish_q, 0)
    pending.append(give_back(2, dq_s.at[:, mine], dq_s.at[:, theirs], dq_hbm))

    for a in range(2):
        @pl.when((chip < wide) if a == 1 else (chip < wide - 1) | (wrap & (chip < wide)))
        def _():
            sum_up(a, wide - 1, sums[a].at[chip]).wait_recv()
            add_in(a, chip, from_dn[a][wide - 1])

        @pl.when(chip < n - 1)
        def _():
            sum_dn(a, hops_up[a] - 1, chip).wait_recv()
            add_in(a, chip, from_up[a][hops_up[a] - 1])

        if a == 0:
            dk_s[...] = (dk_sum[chip] * scale).astype(jnp.bfloat16)
            pending.append(give_back(3, dk_s.at[mine], dk_s.at[theirs], dk_hbm))
        else:
            dv_s[...] = dv_sum[chip].astype(jnp.bfloat16)
            pending.append(give_back(4, dv_s.at[mine], dv_s.at[theirs], dv_hbm))

    for i in range(4):
        swaps[i].wait_send()
    for a in range(2):
        for step in range(hops_up[a]):
            @pl.when(sends_up(a, step))
            def _():
                kv_up(a, step, 0).wait_send()

            @pl.when(gives_dn(a, step))
            def _():
                sum_dn(a, step, 0).wait_send()

        for step in range(hops_dn[a]):
            @pl.when(sends_dn(a, step))
            def _():
                kv_dn(a, step, 0).wait_send()

        for step in range(wide):
            @pl.when(gives_up(a, step))
            def _():
                sum_up(a, step, sums[a].at[0]).wait_send()

    for swap, keep in pending:
        keep.wait()
        swap.wait()


def solution(mesh):
    chips = mesh.shape["cp"] // 2

    def attention_shard(queries, keys, values, out_grad):
        batch, tokens, heads, head_dim = queries.shape
        chunk = 2 * tokens
        half = chips // 2
        bf16, f32 = jnp.bfloat16, jnp.float32
        q = jnp.transpose(queries, (0, 2, 1, 3))
        g = jnp.transpose(out_grad, (0, 2, 1, 3))
        k = keys.reshape(batch, tokens, head_dim)
        v = values.reshape(batch, tokens, head_dim)
        any_spec = pl.BlockSpec(memory_space=pl.ANY)
        dma = pltpu.SemaphoreType.DMA
        out, lse, dq, dk, dv = pl.pallas_call(
            functools.partial(attention_kernel, chips, head_dim ** -0.5),
            out_shape=(
                jax.ShapeDtypeStruct(q.shape, bf16),
                jax.ShapeDtypeStruct((batch, heads, 1, tokens), f32),
                jax.ShapeDtypeStruct(q.shape, bf16),
                jax.ShapeDtypeStruct(k.shape, bf16),
                jax.ShapeDtypeStruct(k.shape, bf16),
            ),
            in_specs=[any_spec] * 4,
            out_specs=(any_spec,) * 5,
            scratch_shapes=[
                pltpu.VMEM((chips, chunk, head_dim), bf16),
                pltpu.VMEM((chips, chunk, head_dim), bf16),
                pltpu.VMEM((head_dim, chunk), bf16),
                pltpu.VMEM((heads, chunk, head_dim), bf16),
                pltpu.VMEM((heads, head_dim, chunk), bf16),
                pltpu.VMEM((heads, chunk, head_dim), bf16),
                pltpu.VMEM((heads, head_dim, chunk), bf16),
                pltpu.VMEM((heads, head_dim, chunk), f32),
                pltpu.VMEM((heads, 1, chunk), f32),
                pltpu.VMEM((heads, 1, chunk), f32),
                pltpu.VMEM((heads, 1, chunk), f32),
                pltpu.VMEM((heads, 1, chunk), f32),
                pltpu.VMEM((heads, chunk, head_dim), bf16),
                pltpu.VMEM((heads, chunk, head_dim), bf16),
                pltpu.VMEM((chunk, head_dim), bf16),
                pltpu.VMEM((chunk, head_dim), bf16),
                pltpu.VMEM((chips, chunk, head_dim), f32),
                pltpu.VMEM((chips, chunk, head_dim), f32),
                pltpu.VMEM((half, chunk, head_dim), f32),
                pltpu.VMEM((half - 1, chunk, head_dim), f32),
                pltpu.VMEM((half, chunk, head_dim), f32),
                pltpu.VMEM((half, chunk, head_dim), f32),
                dma((4,)), dma((4,)), dma((4,)),
                dma((2, half)), dma((2, half)), dma((2, half)), dma((2, half)),
                dma((2, half)), dma((2, half)), dma((2, half)), dma((2, half)),
                dma((5,)), dma((5,)), dma((5,)), pltpu.SemaphoreType.REGULAR,
            ],
            compiler_params=pltpu.CompilerParams(collective_id=0, has_side_effects=True, vmem_limit_bytes=67043328),
            name="ring_attention",
        )(q, k, v, g)
        back = (0, 2, 1, 3)
        return (
            jnp.transpose(out, back),
            lse.reshape(batch, heads, tokens),
            jnp.transpose(dq, back),
            dk.reshape(keys.shape),
            dv.reshape(values.shape),
        )

    seq_spec = P("dp", "cp")
    return jax.shard_map(attention_shard, mesh=mesh, in_specs=(seq_spec,) * 4, out_specs=(seq_spec, P("dp", None, "cp"), seq_spec, seq_spec, seq_spec), check_vma=False)
```

```python
import functools

import jax
import jax.numpy as jnp
from jax import lax
from jax.experimental import pallas as pl
from jax.experimental.pallas import tpu as pltpu
from jax.sharding import PartitionSpec as P

MESH = pl.DeviceIdType.MESH
LOG2E = 1.4426950408889634
LN2 = 0.6931471805599453
TILE = 256
GO_AT = 1


def attention_kernel(n, scale, q_hbm, k_hbm, v_hbm, g_hbm, out_hbm, lse_hbm, dq_hbm, dk_hbm, dv_hbm,
                     k_all, v_all, turned, q_s, q_t, g_s, g_t, acc, run_m, run_l, delta, lse_s, by_head, q_raw, g_raw, dk_s, dv_s,
                     dk_sum, dv_sum, dk_dn, dv_dn, dk_up, dv_up,
                     load_sem, swap_send, swap_recv, kv_up_send, kv_up_recv, kv_dn_send, kv_dn_recv,
                     dkv_dn_send, dkv_dn_recv, dkv_up_send, dkv_up_recv, store_sem, back_send, back_recv, go_sem):
    heads, chunk, head_dim = q_s.shape
    half = chunk // 2
    tiles = chunk // TILE
    rank = lax.axis_index("cp")
    chip = rank // 2
    core = rank % 2
    other = 1 - core
    peer = 2 * chip + other
    above = 2 * ((chip + 1) % n) + core
    below = 2 * ((chip + n - 1) % n) + core
    mine = pl.ds(pl.multiple_of(core * half, half), half)
    theirs = pl.ds(pl.multiple_of(other * half, half), half)
    hops_up = (n // 2, n - 1 - n // 2)
    hops_dn = (n - 1 - n // 2, n // 2)
    kv_all = (k_all, v_all)
    sums = (dk_sum, dv_sum)
    from_up = (dk_dn, dv_dn)
    from_dn = (dk_up, dv_up)
    fold = scale * LOG2E

    def remote(src, dst, send_sem, recv_sem, device):
        return pltpu.make_async_remote_copy(src_ref=src, dst_ref=dst, send_sem=send_sem, recv_sem=recv_sem, device_id={"cp": device}, device_id_type=MESH)

    barrier = pltpu.get_barrier_semaphore()
    for device in (peer, above, below):
        pl.semaphore_signal(barrier, inc=1, device_id={"cp": device}, device_id_type=MESH)
    pl.semaphore_wait(barrier, 3)

    places = (k_all.at[chip, mine], v_all.at[chip, mine], q_raw.at[core], g_raw.at[core])
    sources = (k_hbm, v_hbm, q_hbm, g_hbm)
    swaps = [remote(sources[i].at[other], places[i], swap_send.at[i], swap_recv.at[i], peer) for i in range(4)]
    loads = [pltpu.make_async_copy(sources[i].at[core], places[i], load_sem.at[i]) for i in range(4)]
    for i in range(4):
        swaps[i].start()
        loads[i].start()

    def arrived(i):
        loads[i].wait()
        swaps[i].wait_recv()

    def kv_up(a, step, j):
        return remote(kv_all[a].at[j], kv_all[a].at[j], kv_up_send.at[a, step], kv_up_recv.at[a, step], above)

    def kv_dn(a, step, j):
        return remote(kv_all[a].at[j], kv_all[a].at[j], kv_dn_send.at[a, step], kv_dn_recv.at[a, step], below)

    def sends_up(a, step):
        return (chip < n - 1) & (chip - step >= 0) & (step < hops_up[a])

    def sends_dn(a, step):
        return ((chip + step) % n < hops_dn[a]) & (step < hops_dn[a])

    def send_own(a):
        @pl.when(sends_up(a, 0))
        def _():
            kv_up(a, 0, chip).start()

        @pl.when(sends_dn(a, 0))
        def _():
            kv_dn(a, 0, chip).start()

    for a in range(2):
        arrived(a)

        @pl.when(core == 0)
        def _():
            send_own(a)

    def take_up(a, step):
        j = chip - 1 - step

        @pl.when((j >= 0) & (step < hops_up[a]))
        def _():
            kv_up(a, step, j).wait_recv()

            @pl.when(sends_up(a, step + 1))
            def _():
                kv_up(a, step + 1, j).start()

    def take_dn(a, step):
        j = (chip + 1 + step) % n

        @pl.when((j < hops_dn[a]) & (step < hops_dn[a]))
        def _():
            kv_dn(a, step, j).wait_recv()

            @pl.when(sends_dn(a, step + 1))
            def _():
                kv_dn(a, step + 1, j).start()

    def turn(ref, j):
        for i in range(tiles):
            turned[:, i * TILE:(i + 1) * TILE] = ref[j, i * TILE:(i + 1) * TILE, :].T

    def causal(rows, i):
        key = lax.broadcasted_iota(jnp.int32, (rows, TILE), 0)
        query = lax.broadcasted_iota(jnp.int32, (rows, TILE), 1) + i * TILE
        return key <= query

    def forward_chunk(j, diagonal):
        turn(v_all, j)

        def head(h, _):
            for i in range(tiles):
                cols = slice(i * TILE, (i + 1) * TILE)
                rows = (i + 1) * TILE if diagonal else chunk
                s = jnp.dot(k_all[j, :rows, :], q_t[h, :, cols], preferred_element_type=jnp.float32) * fold
                if diagonal:
                    s = jnp.where(causal(rows, i), s, -jnp.inf)
                    top = jnp.max(s, axis=0, keepdims=True)
                else:
                    old = run_m[h, :, cols]
                    top = jnp.maximum(old, jnp.max(s, axis=0, keepdims=True))
                p = jnp.exp2(s - top)
                total = jnp.sum(p, axis=0, keepdims=True)
                part = jnp.dot(turned[:, :rows], p.astype(jnp.bfloat16), preferred_element_type=jnp.float32)
                run_m[h, :, cols] = top
                if diagonal:
                    run_l[h, :, cols] = total
                    acc[h, :, cols] = part
                else:
                    alpha = jnp.exp2(old - top)
                    run_l[h, :, cols] = run_l[h, :, cols] * alpha + total
                    acc[h, :, cols] = acc[h, :, cols] * alpha + part
            return 0

        lax.fori_loop(0, heads, head, 0, unroll=True)

    def split_heads(src, dst):
        for i in range(2):
            dst[:, i * half:(i + 1) * half, :] = jnp.swapaxes(src[i], 0, 1)

    def join_heads(src, dst):
        for i in range(2):
            dst[i] = jnp.swapaxes(src[:, i * half:(i + 1) * half, :], 0, 1)

    arrived(2)
    split_heads(q_raw, q_s)

    def turn_q(h, _):
        for i in range(tiles):
            cols = slice(i * TILE, (i + 1) * TILE)
            q_t[h, :, cols] = q_s[h, cols, :].T
        return 0

    lax.fori_loop(0, heads, turn_q, 0)
    forward_chunk(chip, True)
    arrived(3)
    split_heads(g_raw, g_s)

    def turn_g(h, _):
        for i in range(tiles):
            cols = slice(i * TILE, (i + 1) * TILE)
            g_t[h, :, cols] = g_s[h, cols, :].T
        return 0

    lax.fori_loop(0, heads, turn_g, 0)

    @pl.when(core == 1)
    def _():
        pl.semaphore_wait(go_sem, 1)
        send_own(0)
        send_own(1)

    def forward_step(step, _):
        for a in range(2):
            take_up(a, step)
            take_dn(a, step)

        @pl.when((core == 0) & (step == GO_AT))
        def _():
            pl.semaphore_signal(go_sem, inc=1, device_id={"cp": peer}, device_id_type=MESH)

        def use(side, _):
            j = jnp.where(side == 0, chip - 1 - step, (chip + 1 + step) % n)
            valid = (j >= 0) & (j < chip) & ((side == 0) | ((j < hops_dn[0]) & (step < hops_dn[0])))

            @pl.when(valid)
            def _():
                forward_chunk(j, False)

            return 0

        lax.fori_loop(0, 2, use, 0)
        return 0

    lax.fori_loop(0, n // 2, forward_step, 0)

    def finish(h, _):
        for i in range(tiles):
            cols = slice(i * TILE, (i + 1) * TILE)
            total = run_l[h, :, cols]
            out = (acc[h, :, cols] / total).astype(jnp.bfloat16)
            acc[h, :, cols] = jnp.zeros((head_dim, TILE), jnp.float32)
            delta[h, :, cols] = jnp.sum(g_t[h, :, cols].astype(jnp.float32) * out.astype(jnp.float32), axis=0, keepdims=True)
            lse2 = run_m[h, :, cols] + jnp.log2(total)
            run_m[h, :, cols] = lse2
            lse_s[h, :, cols] = lse2 * LN2
            by_head[h, cols, :] = out.T
        return 0

    lax.fori_loop(0, heads, finish, 0)
    join_heads(by_head, q_raw)

    def give_back(i, src_mine, src_theirs, dst):
        swap = remote(src_theirs, dst.at[core], back_send.at[i], back_recv.at[i], peer)
        keep = pltpu.make_async_copy(src_mine, dst.at[core], store_sem.at[i])
        swap.start()
        keep.start()
        return swap, keep

    pending = [
        give_back(0, q_raw.at[core], q_raw.at[other], out_hbm),
        give_back(1, lse_s.at[:, :, mine], lse_s.at[:, :, theirs], lse_hbm),
    ]

    def backward_chunk(j, diagonal):
        turn(k_all, j)
        dk_sum[j] = jnp.zeros((chunk, head_dim), jnp.float32)
        dv_sum[j] = jnp.zeros((chunk, head_dim), jnp.float32)

        def head(h, _):
            size = [(i + 1) * TILE if diagonal else chunk for i in range(tiles)]
            cols = [slice(i * TILE, (i + 1) * TILE) for i in range(tiles)]
            ps, dss = [], []
            for i in range(tiles):
                s = jnp.dot(k_all[j, :size[i], :], q_t[h, :, cols[i]], preferred_element_type=jnp.float32)
                dp = jnp.dot(v_all[j, :size[i], :], g_t[h, :, cols[i]], preferred_element_type=jnp.float32)
                if diagonal:
                    s = jnp.where(causal(size[i], i), s, -jnp.inf)
                p = jnp.exp2(s * fold - run_m[h, :, cols[i]])
                ps.append(p.astype(jnp.bfloat16))
                dss.append((p * (dp - delta[h, :, cols[i]])).astype(jnp.bfloat16))
            if diagonal:
                for i in range(tiles):
                    dv_sum[j, :size[i], :] += jnp.dot(ps[i], g_s[h, cols[i], :], preferred_element_type=jnp.float32)
                    dk_sum[j, :size[i], :] += jnp.dot(dss[i], q_s[h, cols[i], :], preferred_element_type=jnp.float32)
                    acc[h, :, cols[i]] += jnp.dot(turned[:, :size[i]], dss[i], preferred_element_type=jnp.float32)
            else:
                pp = jnp.concatenate(ps, axis=1)
                dd = jnp.concatenate(dss, axis=1)
                dv_sum[j] += jnp.dot(pp, g_s[h], preferred_element_type=jnp.float32)
                dk_sum[j] += jnp.dot(dd, q_s[h], preferred_element_type=jnp.float32)
                acc[h] += jnp.dot(turned[...], dd, preferred_element_type=jnp.float32)
            return 0

        lax.fori_loop(0, heads, head, 0, unroll=2)

    def sum_dn(a, step, j):
        return remote(sums[a].at[j], from_up[a].at[step], dkv_dn_send.at[a, step], dkv_dn_recv.at[a, step], below)

    def sum_up(a, step, src):
        return remote(src, from_dn[a].at[step], dkv_up_send.at[a, step], dkv_up_recv.at[a, step], above)

    wide = n // 2
    wrap = False

    def gives_dn(a, step):
        skip = (a == 0) & (step == 0) & (chip == n - 1) & wrap
        return (chip - hops_up[a] + step >= 0) & (step < hops_up[a]) & jnp.logical_not(skip)

    def gets_dn(a, step):
        skip = (a == 0) & (step == 1) & (chip == n - 2) & wrap
        return (step >= 1) & (chip < n - 1) & jnp.logical_not(skip)

    def up_index(step):
        return (chip + wide - step + n) % n

    def gives_up(a, step):
        j = up_index(step)
        in_reach = (j < wide) & (j != chip) & (step < wide)
        if a == 0:
            in_reach &= (wrap & (chip == n - 1)) | ((step >= 1) & (wrap | (j < wide - 1)))
        return in_reach

    def gets_up(a, step):
        return (step >= 2 - a) | ((step >= 1) & (up_index(step) > chip))

    def add_in(a, j, part):
        sums[a][j] = sums[a][j] + part

    def pass_dn(a, step):
        @pl.when(gives_dn(a, step))
        def _():
            j = chip - hops_up[a] + step

            before = jnp.maximum(step - 1, 0)

            @pl.when(gets_dn(a, step))
            def _():
                sum_dn(a, before, j).wait_recv()
                add_in(a, j, from_up[a][before])

            sum_dn(a, step, j).start()

    def pass_up(a, step):
        @pl.when(gives_up(a, step))
        def _():
            j = up_index(step)
            before = jnp.maximum(step - 1, 0)

            @pl.when(gets_up(a, step))
            def _():
                sum_up(a, before, sums[a].at[j]).wait_recv()

            @pl.when(j < chip)
            def _():
                @pl.when(gets_up(a, step))
                def _():
                    add_in(a, j, from_dn[a][before])

                sum_up(a, step, sums[a].at[j]).start()

            @pl.when(j > chip)
            def _():
                sum_up(a, step, from_dn[a].at[before]).start()

    def backward_pos(s, _):
        step = jnp.maximum(s - 1, 0) // 2
        first = s == 0
        down = s % 2 == 1
        near = chip - hops_up[1] + step
        far = up_index(step + 1)
        j = jnp.where(first, chip - n // 2, jnp.where(down, near, far))
        valid = (j >= 0) & (j < chip) & (first | down | (j < wide))

        @pl.when(valid)
        def _():
            backward_chunk(j, False)

        @pl.when(first)
        def _():
            pass_dn(0, 0)
            pass_up(0, 0)
            pass_up(1, 0)

        @pl.when(down)
        def _():
            pass_dn(0, step + 1)
            pass_dn(1, step)

        @pl.when(jnp.logical_not(first | down))
        def _():
            pass_up(0, step + 1)
            pass_up(1, step + 1)

        @pl.when(s == n // 2 - 1)
        def _():
            backward_chunk(chip, True)

        return 0

    lax.fori_loop(0, n - 1, backward_pos, 0)

    def finish_q(h, _):
        for i in range(tiles):
            cols = slice(i * TILE, (i + 1) * TILE)
            by_head[h, cols, :] = (acc[h, :, cols] * scale).astype(jnp.bfloat16).T
        return 0

    lax.fori_loop(0, heads, finish_q, 0)
    join_heads(by_head, g_raw)
    pending.append(give_back(2, g_raw.at[core], g_raw.at[other], dq_hbm))

    for a in range(2):
        @pl.when((chip < wide) if a == 1 else (chip < wide - 1) | (wrap & (chip < wide)))
        def _():
            sum_up(a, wide - 1, sums[a].at[chip]).wait_recv()
            add_in(a, chip, from_dn[a][wide - 1])

        @pl.when(chip < n - 1)
        def _():
            sum_dn(a, hops_up[a] - 1, chip).wait_recv()
            add_in(a, chip, from_up[a][hops_up[a] - 1])

        if a == 0:
            dk_s[...] = (dk_sum[chip] * scale).astype(jnp.bfloat16)
            pending.append(give_back(3, dk_s.at[mine], dk_s.at[theirs], dk_hbm))
        else:
            dv_s[...] = dv_sum[chip].astype(jnp.bfloat16)
            pending.append(give_back(4, dv_s.at[mine], dv_s.at[theirs], dv_hbm))

    for i in range(4):
        swaps[i].wait_send()
    for a in range(2):
        for step in range(hops_up[a]):
            @pl.when(sends_up(a, step))
            def _():
                kv_up(a, step, 0).wait_send()

            @pl.when(gives_dn(a, step))
            def _():
                sum_dn(a, step, 0).wait_send()

        for step in range(hops_dn[a]):
            @pl.when(sends_dn(a, step))
            def _():
                kv_dn(a, step, 0).wait_send()

        for step in range(wide):
            @pl.when(gives_up(a, step))
            def _():
                sum_up(a, step, sums[a].at[0]).wait_send()

    for swap, keep in pending:
        keep.wait()
        swap.wait()


def solution(mesh):
    chips = mesh.shape["cp"] // 2

    def attention_shard(queries, keys, values, out_grad):
        batch, tokens, heads, head_dim = queries.shape
        chunk = 2 * tokens
        half = chips // 2
        bf16, f32 = jnp.bfloat16, jnp.float32
        k = keys.reshape(batch, tokens, head_dim)
        v = values.reshape(batch, tokens, head_dim)
        any_spec = pl.BlockSpec(memory_space=pl.ANY)
        dma = pltpu.SemaphoreType.DMA
        out, lse, dq, dk, dv = pl.pallas_call(
            functools.partial(attention_kernel, chips, head_dim ** -0.5),
            out_shape=(
                jax.ShapeDtypeStruct(queries.shape, bf16),
                jax.ShapeDtypeStruct((batch, heads, 1, tokens), f32),
                jax.ShapeDtypeStruct(queries.shape, bf16),
                jax.ShapeDtypeStruct(k.shape, bf16),
                jax.ShapeDtypeStruct(k.shape, bf16),
            ),
            in_specs=[any_spec] * 4,
            out_specs=(any_spec,) * 5,
            scratch_shapes=[
                pltpu.VMEM((chips, chunk, head_dim), bf16),
                pltpu.VMEM((chips, chunk, head_dim), bf16),
                pltpu.VMEM((head_dim, chunk), bf16),
                pltpu.VMEM((heads, chunk, head_dim), bf16),
                pltpu.VMEM((heads, head_dim, chunk), bf16),
                pltpu.VMEM((heads, chunk, head_dim), bf16),
                pltpu.VMEM((heads, head_dim, chunk), bf16),
                pltpu.VMEM((heads, head_dim, chunk), f32),
                pltpu.VMEM((heads, 1, chunk), f32),
                pltpu.VMEM((heads, 1, chunk), f32),
                pltpu.VMEM((heads, 1, chunk), f32),
                pltpu.VMEM((heads, 1, chunk), f32),
                pltpu.VMEM((heads, chunk, head_dim), bf16),
                pltpu.VMEM((2, tokens, heads, head_dim), bf16),
                pltpu.VMEM((2, tokens, heads, head_dim), bf16),
                pltpu.VMEM((chunk, head_dim), bf16),
                pltpu.VMEM((chunk, head_dim), bf16),
                pltpu.VMEM((chips, chunk, head_dim), f32),
                pltpu.VMEM((chips, chunk, head_dim), f32),
                pltpu.VMEM((half, chunk, head_dim), f32),
                pltpu.VMEM((half - 1, chunk, head_dim), f32),
                pltpu.VMEM((half, chunk, head_dim), f32),
                pltpu.VMEM((half, chunk, head_dim), f32),
                dma((4,)), dma((4,)), dma((4,)),
                dma((2, half)), dma((2, half)), dma((2, half)), dma((2, half)),
                dma((2, half)), dma((2, half)), dma((2, half)), dma((2, half)),
                dma((5,)), dma((5,)), dma((5,)), pltpu.SemaphoreType.REGULAR,
            ],
            compiler_params=pltpu.CompilerParams(collective_id=0, has_side_effects=True, vmem_limit_bytes=67043328),
            name="ring_attention",
        )(queries, k, v, out_grad)
        return (
            out,
            lse.reshape(batch, heads, tokens),
            dq,
            dk.reshape(keys.shape),
            dv.reshape(values.shape),
        )

    seq_spec = P("dp", "cp")
    return jax.shard_map(attention_shard, mesh=mesh, in_specs=(seq_spec,) * 4, out_specs=(seq_spec, P("dp", None, "cp"), seq_spec, seq_spec, seq_spec), check_vma=False)
```

```python
import functools

import jax
import jax.numpy as jnp
from jax import lax
from jax.experimental import pallas as pl
from jax.experimental.pallas import tpu as pltpu
from jax.sharding import PartitionSpec as P

MESH = pl.DeviceIdType.MESH
LOG2E = 1.4426950408889634
LN2 = 0.6931471805599453
TILE = 256
GO_AT = 2


def attention_kernel(n, scale, q_hbm, k_hbm, v_hbm, g_hbm, out_hbm, lse_hbm, dq_hbm, dk_hbm, dv_hbm,
                     k_all, v_all, turned, q_s, q_t, g_s, g_t, acc, run_m, run_l, delta, lse_s, by_head, q_raw, g_raw, dk_s, dv_s,
                     dk_sum, dv_sum, dk_dn, dv_dn, dk_up, dv_up,
                     load_sem, swap_send, swap_recv, kv_up_send, kv_up_recv, kv_dn_send, kv_dn_recv,
                     dkv_dn_send, dkv_dn_recv, dkv_up_send, dkv_up_recv, store_sem, back_send, back_recv, go_sem):
    heads, chunk, head_dim = q_s.shape
    half = chunk // 2
    tiles = chunk // TILE
    rank = lax.axis_index("cp")
    chip = rank // 2
    core = rank % 2
    other = 1 - core
    peer = 2 * chip + other
    above = 2 * ((chip + 1) % n) + core
    below = 2 * ((chip + n - 1) % n) + core
    mine = pl.ds(pl.multiple_of(core * half, half), half)
    theirs = pl.ds(pl.multiple_of(other * half, half), half)
    hops_up = (n // 2, n - 1 - n // 2)
    hops_dn = (n - 1 - n // 2, n // 2)
    kv_all = (k_all, v_all)
    sums = (dk_sum, dv_sum)
    from_up = (dk_dn, dv_dn)
    from_dn = (dk_up, dv_up)
    fold = scale * LOG2E

    def remote(src, dst, send_sem, recv_sem, device):
        return pltpu.make_async_remote_copy(src_ref=src, dst_ref=dst, send_sem=send_sem, recv_sem=recv_sem, device_id={"cp": device}, device_id_type=MESH)

    barrier = pltpu.get_barrier_semaphore()
    for device in (peer, above, below):
        pl.semaphore_signal(barrier, inc=1, device_id={"cp": device}, device_id_type=MESH)
    pl.semaphore_wait(barrier, 3)

    places = (k_all.at[chip, mine], v_all.at[chip, mine], q_raw.at[core], g_raw.at[core])
    sources = (k_hbm, v_hbm, q_hbm, g_hbm)
    swaps = [remote(sources[i].at[other], places[i], swap_send.at[i], swap_recv.at[i], peer) for i in range(4)]
    loads = [pltpu.make_async_copy(sources[i].at[core], places[i], load_sem.at[i]) for i in range(4)]
    for i in range(4):
        swaps[i].start()
        loads[i].start()

    def arrived(i):
        loads[i].wait()
        swaps[i].wait_recv()

    def kv_up(a, step, j):
        return remote(kv_all[a].at[j], kv_all[a].at[j], kv_up_send.at[a, step], kv_up_recv.at[a, step], above)

    def kv_dn(a, step, j):
        return remote(kv_all[a].at[j], kv_all[a].at[j], kv_dn_send.at[a, step], kv_dn_recv.at[a, step], below)

    def sends_up(a, step):
        return (chip < n - 1) & (chip - step >= 0) & (step < hops_up[a])

    def sends_dn(a, step):
        return ((chip + step) % n < hops_dn[a]) & (step < hops_dn[a])

    def send_own(a):
        @pl.when(sends_up(a, 0))
        def _():
            kv_up(a, 0, chip).start()

        @pl.when(sends_dn(a, 0))
        def _():
            kv_dn(a, 0, chip).start()

    for a in range(2):
        arrived(a)

        @pl.when(core == 0)
        def _():
            send_own(a)

    def take_up(a, step):
        j = chip - 1 - step

        @pl.when((j >= 0) & (step < hops_up[a]))
        def _():
            kv_up(a, step, j).wait_recv()

            @pl.when(sends_up(a, step + 1))
            def _():
                kv_up(a, step + 1, j).start()

    def take_dn(a, step):
        j = (chip + 1 + step) % n

        @pl.when((j < hops_dn[a]) & (step < hops_dn[a]))
        def _():
            kv_dn(a, step, j).wait_recv()

            @pl.when(sends_dn(a, step + 1))
            def _():
                kv_dn(a, step + 1, j).start()

    def turn(ref, j):
        for i in range(tiles):
            turned[:, i * TILE:(i + 1) * TILE] = ref[j, i * TILE:(i + 1) * TILE, :].T

    def causal(rows, i):
        key = lax.broadcasted_iota(jnp.int32, (rows, TILE), 0)
        query = lax.broadcasted_iota(jnp.int32, (rows, TILE), 1) + i * TILE
        return key <= query

    def forward_chunk(j, diagonal):
        turn(v_all, j)

        def head(h, _):
            for i in range(tiles):
                cols = slice(i * TILE, (i + 1) * TILE)
                rows = (i + 1) * TILE if diagonal else chunk
                s = jnp.dot(k_all[j, :rows, :], q_t[h, :, cols], preferred_element_type=jnp.float32) * fold
                if diagonal:
                    s = jnp.where(causal(rows, i), s, -jnp.inf)
                    top = jnp.max(s, axis=0, keepdims=True)
                else:
                    old = run_m[h, :, cols]
                    top = jnp.maximum(old, jnp.max(s, axis=0, keepdims=True))
                p = jnp.exp2(s - top)
                total = jnp.sum(p, axis=0, keepdims=True)
                part = jnp.dot(turned[:, :rows], p.astype(jnp.bfloat16), preferred_element_type=jnp.float32)
                run_m[h, :, cols] = top
                if diagonal:
                    run_l[h, :, cols] = total
                    acc[h, :, cols] = part
                else:
                    alpha = jnp.exp2(old - top)
                    run_l[h, :, cols] = run_l[h, :, cols] * alpha + total
                    acc[h, :, cols] = acc[h, :, cols] * alpha + part
            return 0

        lax.fori_loop(0, heads, head, 0, unroll=True)

    def split_heads(src, dst):
        for i in range(2):
            dst[:, i * half:(i + 1) * half, :] = jnp.swapaxes(src[i], 0, 1)

    def join_heads(src, dst):
        for i in range(2):
            dst[i] = jnp.swapaxes(src[:, i * half:(i + 1) * half, :], 0, 1)

    arrived(2)
    split_heads(q_raw, q_s)

    def turn_q(h, _):
        for i in range(tiles):
            cols = slice(i * TILE, (i + 1) * TILE)
            q_t[h, :, cols] = q_s[h, cols, :].T
        return 0

    lax.fori_loop(0, heads, turn_q, 0)
    forward_chunk(chip, True)
    arrived(3)
    split_heads(g_raw, g_s)

    def turn_g(h, _):
        for i in range(tiles):
            cols = slice(i * TILE, (i + 1) * TILE)
            g_t[h, :, cols] = g_s[h, cols, :].T
        return 0

    lax.fori_loop(0, heads, turn_g, 0)

    @pl.when(core == 1)
    def _():
        pl.semaphore_wait(go_sem, 1)
        send_own(0)
        send_own(1)

    def forward_step(step, _):
        for a in range(2):
            take_up(a, step)
            take_dn(a, step)

        @pl.when((core == 0) & (step == GO_AT))
        def _():
            pl.semaphore_signal(go_sem, inc=1, device_id={"cp": peer}, device_id_type=MESH)

        def use(side, _):
            j = jnp.where(side == 0, chip - 1 - step, (chip + 1 + step) % n)
            valid = (j >= 0) & (j < chip) & ((side == 0) | ((j < hops_dn[0]) & (step < hops_dn[0])))

            @pl.when(valid)
            def _():
                forward_chunk(j, False)

            return 0

        lax.fori_loop(0, 2, use, 0)
        return 0

    lax.fori_loop(0, n // 2, forward_step, 0)

    def finish(h, _):
        for i in range(tiles):
            cols = slice(i * TILE, (i + 1) * TILE)
            total = run_l[h, :, cols]
            out = (acc[h, :, cols] / total).astype(jnp.bfloat16)
            acc[h, :, cols] = jnp.zeros((head_dim, TILE), jnp.float32)
            delta[h, :, cols] = jnp.sum(g_t[h, :, cols].astype(jnp.float32) * out.astype(jnp.float32), axis=0, keepdims=True)
            lse2 = run_m[h, :, cols] + jnp.log2(total)
            run_m[h, :, cols] = lse2
            lse_s[h, :, cols] = lse2 * LN2
            by_head[h, cols, :] = out.T
        return 0

    lax.fori_loop(0, heads, finish, 0)
    join_heads(by_head, q_raw)

    def give_back(i, src_mine, src_theirs, dst):
        swap = remote(src_theirs, dst.at[core], back_send.at[i], back_recv.at[i], peer)
        keep = pltpu.make_async_copy(src_mine, dst.at[core], store_sem.at[i])
        swap.start()
        keep.start()
        return swap, keep

    pending = [
        give_back(0, q_raw.at[core], q_raw.at[other], out_hbm),
        give_back(1, lse_s.at[:, :, mine], lse_s.at[:, :, theirs], lse_hbm),
    ]

    def backward_chunk(j, diagonal):
        turn(k_all, j)
        dk_sum[j] = jnp.zeros((chunk, head_dim), jnp.float32)
        dv_sum[j] = jnp.zeros((chunk, head_dim), jnp.float32)

        def head(h, _):
            size = [(i + 1) * TILE if diagonal else chunk for i in range(tiles)]
            cols = [slice(i * TILE, (i + 1) * TILE) for i in range(tiles)]
            ps, dss = [], []
            for i in range(tiles):
                s = jnp.dot(k_all[j, :size[i], :], q_t[h, :, cols[i]], preferred_element_type=jnp.float32)
                dp = jnp.dot(v_all[j, :size[i], :], g_t[h, :, cols[i]], preferred_element_type=jnp.float32)
                if diagonal:
                    s = jnp.where(causal(size[i], i), s, -jnp.inf)
                p = jnp.exp2(s * fold - run_m[h, :, cols[i]])
                ps.append(p.astype(jnp.bfloat16))
                dss.append((p * (dp - delta[h, :, cols[i]])).astype(jnp.bfloat16))
            if diagonal:
                for i in range(tiles):
                    dv_sum[j, :size[i], :] += jnp.dot(ps[i], g_s[h, cols[i], :], preferred_element_type=jnp.float32)
                    dk_sum[j, :size[i], :] += jnp.dot(dss[i], q_s[h, cols[i], :], preferred_element_type=jnp.float32)
                    acc[h, :, cols[i]] += jnp.dot(turned[:, :size[i]], dss[i], preferred_element_type=jnp.float32)
            else:
                pp = jnp.concatenate(ps, axis=1)
                dd = jnp.concatenate(dss, axis=1)
                dv_sum[j] += jnp.dot(pp, g_s[h], preferred_element_type=jnp.float32)
                dk_sum[j] += jnp.dot(dd, q_s[h], preferred_element_type=jnp.float32)
                acc[h] += jnp.dot(turned[...], dd, preferred_element_type=jnp.float32)
            return 0

        lax.fori_loop(0, heads, head, 0, unroll=2)

    def sum_dn(a, step, j):
        return remote(sums[a].at[j], from_up[a].at[step], dkv_dn_send.at[a, step], dkv_dn_recv.at[a, step], below)

    def sum_up(a, step, src):
        return remote(src, from_dn[a].at[step], dkv_up_send.at[a, step], dkv_up_recv.at[a, step], above)

    wide = n // 2
    wrap = False

    def gives_dn(a, step):
        skip = (a == 0) & (step == 0) & (chip == n - 1) & wrap
        return (chip - hops_up[a] + step >= 0) & (step < hops_up[a]) & jnp.logical_not(skip)

    def gets_dn(a, step):
        skip = (a == 0) & (step == 1) & (chip == n - 2) & wrap
        return (step >= 1) & (chip < n - 1) & jnp.logical_not(skip)

    def up_index(step):
        return (chip + wide - step + n) % n

    def gives_up(a, step):
        j = up_index(step)
        in_reach = (j < wide) & (j != chip) & (step < wide)
        if a == 0:
            in_reach &= (wrap & (chip == n - 1)) | ((step >= 1) & (wrap | (j < wide - 1)))
        return in_reach

    def gets_up(a, step):
        return (step >= 2 - a) | ((step >= 1) & (up_index(step) > chip))

    def add_in(a, j, part):
        sums[a][j] = sums[a][j] + part

    def pass_dn(a, step):
        @pl.when(gives_dn(a, step))
        def _():
            j = chip - hops_up[a] + step

            before = jnp.maximum(step - 1, 0)

            @pl.when(gets_dn(a, step))
            def _():
                sum_dn(a, before, j).wait_recv()
                add_in(a, j, from_up[a][before])

            sum_dn(a, step, j).start()

    def pass_up(a, step):
        @pl.when(gives_up(a, step))
        def _():
            j = up_index(step)
            before = jnp.maximum(step - 1, 0)

            @pl.when(gets_up(a, step))
            def _():
                sum_up(a, before, sums[a].at[j]).wait_recv()

            @pl.when(j < chip)
            def _():
                @pl.when(gets_up(a, step))
                def _():
                    add_in(a, j, from_dn[a][before])

                sum_up(a, step, sums[a].at[j]).start()

            @pl.when(j > chip)
            def _():
                sum_up(a, step, from_dn[a].at[before]).start()

    def backward_pos(s, _):
        step = jnp.maximum(s - 1, 0) // 2
        first = s == 0
        down = s % 2 == 1
        near = chip - hops_up[1] + step
        far = up_index(step + 1)
        j = jnp.where(first, chip - n // 2, jnp.where(down, near, far))
        valid = (j >= 0) & (j < chip) & (first | down | (j < wide))

        @pl.when(valid)
        def _():
            backward_chunk(j, False)

        @pl.when(first)
        def _():
            pass_dn(0, 0)
            pass_up(0, 0)
            pass_up(1, 0)

        @pl.when(down)
        def _():
            pass_dn(0, step + 1)
            pass_dn(1, step)

        @pl.when(jnp.logical_not(first | down))
        def _():
            pass_up(0, step + 1)
            pass_up(1, step + 1)

        @pl.when(s == n // 2 - 1)
        def _():
            backward_chunk(chip, True)

        return 0

    lax.fori_loop(0, n - 1, backward_pos, 0)

    def finish_q(h, _):
        for i in range(tiles):
            cols = slice(i * TILE, (i + 1) * TILE)
            by_head[h, cols, :] = (acc[h, :, cols] * scale).astype(jnp.bfloat16).T
        return 0

    lax.fori_loop(0, heads, finish_q, 0)
    join_heads(by_head, g_raw)
    pending.append(give_back(2, g_raw.at[core], g_raw.at[other], dq_hbm))

    for a in range(2):
        @pl.when((chip < wide) if a == 1 else (chip < wide - 1) | (wrap & (chip < wide)))
        def _():
            sum_up(a, wide - 1, sums[a].at[chip]).wait_recv()
            add_in(a, chip, from_dn[a][wide - 1])

        @pl.when(chip < n - 1)
        def _():
            sum_dn(a, hops_up[a] - 1, chip).wait_recv()
            add_in(a, chip, from_up[a][hops_up[a] - 1])

        if a == 0:
            dk_s[...] = (dk_sum[chip] * scale).astype(jnp.bfloat16)
            pending.append(give_back(3, dk_s.at[mine], dk_s.at[theirs], dk_hbm))
        else:
            dv_s[...] = dv_sum[chip].astype(jnp.bfloat16)
            pending.append(give_back(4, dv_s.at[mine], dv_s.at[theirs], dv_hbm))

    for i in range(4):
        swaps[i].wait_send()
    for a in range(2):
        for step in range(hops_up[a]):
            @pl.when(sends_up(a, step))
            def _():
                kv_up(a, step, 0).wait_send()

            @pl.when(gives_dn(a, step))
            def _():
                sum_dn(a, step, 0).wait_send()

        for step in range(hops_dn[a]):
            @pl.when(sends_dn(a, step))
            def _():
                kv_dn(a, step, 0).wait_send()

        for step in range(wide):
            @pl.when(gives_up(a, step))
            def _():
                sum_up(a, step, sums[a].at[0]).wait_send()

    for swap, keep in pending:
        keep.wait()
        swap.wait()


def place_kernel(lse_in, out_in, dq_in, dk_in, dv_in, lse_out, out_out, dq_out, dk_out, dv_out, out_buf, dq_buf, dk_buf, dv_buf, in_sem, out_sem):
    pieces = []
    for src, buf, dst in ((out_in, out_buf, out_out), (dq_in, dq_buf, dq_out), (dk_in, dk_buf, dk_out), (dv_in, dv_buf, dv_out)):
        for b in range(src.shape[0]):
            i = len(pieces)
            pieces.append((pltpu.make_async_copy(src.at[b], buf.at[b], in_sem.at[i]), pltpu.make_async_copy(buf.at[b], dst.at[b], out_sem.at[i])))
    for load, _ in pieces:
        load.start()
    lse_out[...] = lse_in[:, :, 0, :]
    for load, store in pieces:
        load.wait()
        store.start()
    for _, store in pieces:
        store.wait()


def solution(mesh):
    chips = mesh.shape["cp"] // 2

    def attention_shard(queries, keys, values, out_grad):
        batch, tokens, heads, head_dim = queries.shape
        chunk = 2 * tokens
        half = chips // 2
        bf16, f32 = jnp.bfloat16, jnp.float32
        k = keys.reshape(batch, tokens, head_dim)
        v = values.reshape(batch, tokens, head_dim)
        any_spec = pl.BlockSpec(memory_space=pl.ANY)
        dma = pltpu.SemaphoreType.DMA
        out, lse, dq, dk, dv = pl.pallas_call(
            functools.partial(attention_kernel, chips, head_dim ** -0.5),
            out_shape=(
                jax.ShapeDtypeStruct(queries.shape, bf16),
                jax.ShapeDtypeStruct((batch, heads, 1, tokens), f32),
                jax.ShapeDtypeStruct(queries.shape, bf16),
                jax.ShapeDtypeStruct(k.shape, bf16),
                jax.ShapeDtypeStruct(k.shape, bf16),
            ),
            in_specs=[any_spec] * 4,
            out_specs=(any_spec,) * 5,
            scratch_shapes=[
                pltpu.VMEM((chips, chunk, head_dim), bf16),
                pltpu.VMEM((chips, chunk, head_dim), bf16),
                pltpu.VMEM((head_dim, chunk), bf16),
                pltpu.VMEM((heads, chunk, head_dim), bf16),
                pltpu.VMEM((heads, head_dim, chunk), bf16),
                pltpu.VMEM((heads, chunk, head_dim), bf16),
                pltpu.VMEM((heads, head_dim, chunk), bf16),
                pltpu.VMEM((heads, head_dim, chunk), f32),
                pltpu.VMEM((heads, 1, chunk), f32),
                pltpu.VMEM((heads, 1, chunk), f32),
                pltpu.VMEM((heads, 1, chunk), f32),
                pltpu.VMEM((heads, 1, chunk), f32),
                pltpu.VMEM((heads, chunk, head_dim), bf16),
                pltpu.VMEM((2, tokens, heads, head_dim), bf16),
                pltpu.VMEM((2, tokens, heads, head_dim), bf16),
                pltpu.VMEM((chunk, head_dim), bf16),
                pltpu.VMEM((chunk, head_dim), bf16),
                pltpu.VMEM((chips, chunk, head_dim), f32),
                pltpu.VMEM((chips, chunk, head_dim), f32),
                pltpu.VMEM((half, chunk, head_dim), f32),
                pltpu.VMEM((half - 1, chunk, head_dim), f32),
                pltpu.VMEM((half, chunk, head_dim), f32),
                pltpu.VMEM((half, chunk, head_dim), f32),
                dma((4,)), dma((4,)), dma((4,)),
                dma((2, half)), dma((2, half)), dma((2, half)), dma((2, half)),
                dma((2, half)), dma((2, half)), dma((2, half)), dma((2, half)),
                dma((5,)), dma((5,)), dma((5,)), pltpu.SemaphoreType.REGULAR,
            ],
            compiler_params=pltpu.CompilerParams(collective_id=0, has_side_effects=True, vmem_limit_bytes=67043328),
            name="ring_attention",
        )(queries, k, v, out_grad)
        vmem_spec = pl.BlockSpec(memory_space=pltpu.VMEM)
        results = (out, dq, dk, dv)
        row_lse, out, dq, dk, dv = pl.pallas_call(
            place_kernel,
            out_shape=(jax.ShapeDtypeStruct((batch, heads, tokens), f32),) + tuple(jax.ShapeDtypeStruct(x.shape, bf16) for x in results),
            in_specs=[vmem_spec] + [any_spec] * 4,
            out_specs=(vmem_spec,) + (any_spec,) * 4,
            scratch_shapes=[pltpu.VMEM(x.shape, bf16) for x in results] + [dma((4 * batch,)), dma((4 * batch,))],
            name="place_results",
        )(lse, *results)
        return out, row_lse, dq, dk.reshape(keys.shape), dv.reshape(values.shape)

    seq_spec = P("dp", "cp")
    return jax.shard_map(attention_shard, mesh=mesh, in_specs=(seq_spec,) * 4, out_specs=(seq_spec, P("dp", None, "cp"), seq_spec, seq_spec, seq_spec), check_vma=False)
```

```python
import functools

import jax
import jax.numpy as jnp
from jax import lax
from jax.experimental import pallas as pl
from jax.experimental.pallas import tpu as pltpu
from jax.sharding import PartitionSpec as P

MESH = pl.DeviceIdType.MESH
LOG2E = 1.4426950408889634
LN2 = 0.6931471805599453
TILE = 256
GO_AT = 2


def attention_kernel(n, scale, q_hbm, k_hbm, v_hbm, g_hbm, out_hbm, lse_hbm, dq_hbm, dk_hbm, dv_hbm,
                     k_all, v_all, turned, q_s, q_t, g_s, g_t, acc, run_m, run_l, delta, lse_s, by_head, q_raw, g_raw, dk_s, dv_s,
                     dk_sum, dv_sum, dk_dn, dv_dn, dk_up, dv_up,
                     load_sem, swap_send, swap_recv, kv_up_send, kv_up_recv, kv_dn_send, kv_dn_recv,
                     dkv_dn_send, dkv_dn_recv, dkv_up_send, dkv_up_recv, store_sem, back_send, back_recv, go_sem):
    heads, chunk, head_dim = q_s.shape
    half = chunk // 2
    tiles = chunk // TILE
    rank = lax.axis_index("cp")
    chip = rank // 2
    core = rank % 2
    other = 1 - core
    peer = 2 * chip + other
    above = 2 * ((chip + 1) % n) + core
    below = 2 * ((chip + n - 1) % n) + core
    mine = pl.ds(pl.multiple_of(core * half, half), half)
    theirs = pl.ds(pl.multiple_of(other * half, half), half)
    hops_up = (n // 2, n - 1 - n // 2)
    hops_dn = (n - 1 - n // 2, n // 2)
    kv_all = (k_all, v_all)
    sums = (dk_sum, dv_sum)
    from_up = (dk_dn, dv_dn)
    from_dn = (dk_up, dv_up)
    fold = scale * LOG2E

    def remote(src, dst, send_sem, recv_sem, device):
        return pltpu.make_async_remote_copy(src_ref=src, dst_ref=dst, send_sem=send_sem, recv_sem=recv_sem, device_id={"cp": device}, device_id_type=MESH)

    barrier = pltpu.get_barrier_semaphore()
    for device in (peer, above, below):
        pl.semaphore_signal(barrier, inc=1, device_id={"cp": device}, device_id_type=MESH)
    pl.semaphore_wait(barrier, 3)

    places = (k_all.at[chip, mine], v_all.at[chip, mine], q_raw.at[core], g_raw.at[core])
    sources = (k_hbm, v_hbm, q_hbm, g_hbm)
    swaps = [remote(sources[i].at[other], places[i], swap_send.at[i], swap_recv.at[i], peer) for i in range(4)]
    loads = [pltpu.make_async_copy(sources[i].at[core], places[i], load_sem.at[i]) for i in range(4)]
    for i in range(4):
        swaps[i].start()
        loads[i].start()

    def arrived(i):
        loads[i].wait()
        swaps[i].wait_recv()

    def kv_up(a, step, j):
        return remote(kv_all[a].at[j], kv_all[a].at[j], kv_up_send.at[a, step], kv_up_recv.at[a, step], above)

    def kv_dn(a, step, j):
        return remote(kv_all[a].at[j], kv_all[a].at[j], kv_dn_send.at[a, step], kv_dn_recv.at[a, step], below)

    def sends_up(a, step):
        return (chip < n - 1) & (chip - step >= 0) & (step < hops_up[a])

    def sends_dn(a, step):
        return ((chip + step) % n < hops_dn[a]) & (step < hops_dn[a])

    def send_own(a):
        @pl.when(sends_up(a, 0))
        def _():
            kv_up(a, 0, chip).start()

        @pl.when(sends_dn(a, 0))
        def _():
            kv_dn(a, 0, chip).start()

    for a in range(2):
        arrived(a)

        @pl.when(core == 0)
        def _():
            send_own(a)

    def take_up(a, step):
        j = chip - 1 - step

        @pl.when((j >= 0) & (step < hops_up[a]))
        def _():
            kv_up(a, step, j).wait_recv()

            @pl.when(sends_up(a, step + 1))
            def _():
                kv_up(a, step + 1, j).start()

    def take_dn(a, step):
        j = (chip + 1 + step) % n

        @pl.when((j < hops_dn[a]) & (step < hops_dn[a]))
        def _():
            kv_dn(a, step, j).wait_recv()

            @pl.when(sends_dn(a, step + 1))
            def _():
                kv_dn(a, step + 1, j).start()

    def turn(ref, j):
        for i in range(tiles):
            turned[:, i * TILE:(i + 1) * TILE] = ref[j, i * TILE:(i + 1) * TILE, :].T

    def causal(rows, i):
        key = lax.broadcasted_iota(jnp.int32, (rows, TILE), 0)
        query = lax.broadcasted_iota(jnp.int32, (rows, TILE), 1) + i * TILE
        return key <= query

    def forward_chunk(j, diagonal):
        turn(v_all, j)

        def head(h, _):
            for i in range(tiles):
                cols = slice(i * TILE, (i + 1) * TILE)
                rows = (i + 1) * TILE if diagonal else chunk
                s = jnp.dot(k_all[j, :rows, :], q_t[h, :, cols], preferred_element_type=jnp.float32) * fold
                if diagonal:
                    s = jnp.where(causal(rows, i), s, -jnp.inf)
                    top = jnp.max(s, axis=0, keepdims=True)
                else:
                    old = run_m[h, :, cols]
                    top = jnp.maximum(old, jnp.max(s, axis=0, keepdims=True))
                p = jnp.exp2(s - top)
                total = jnp.sum(p, axis=0, keepdims=True)
                part = jnp.dot(turned[:, :rows], p.astype(jnp.bfloat16), preferred_element_type=jnp.float32)
                run_m[h, :, cols] = top
                if diagonal:
                    run_l[h, :, cols] = total
                    acc[h, :, cols] = part
                else:
                    alpha = jnp.exp2(old - top)
                    run_l[h, :, cols] = run_l[h, :, cols] * alpha + total
                    acc[h, :, cols] = acc[h, :, cols] * alpha + part
            return 0

        lax.fori_loop(0, heads, head, 0, unroll=True)

    def split_heads(src, dst):
        for i in range(2):
            dst[:, i * half:(i + 1) * half, :] = jnp.swapaxes(src[i], 0, 1)

    def join_heads(src, dst):
        for i in range(2):
            dst[i] = jnp.swapaxes(src[:, i * half:(i + 1) * half, :], 0, 1)

    arrived(2)
    split_heads(q_raw, q_s)

    def turn_q(h, _):
        for i in range(tiles):
            cols = slice(i * TILE, (i + 1) * TILE)
            q_t[h, :, cols] = q_s[h, cols, :].T
        return 0

    lax.fori_loop(0, heads, turn_q, 0)
    forward_chunk(chip, True)
    arrived(3)
    split_heads(g_raw, g_s)

    def turn_g(h, _):
        for i in range(tiles):
            cols = slice(i * TILE, (i + 1) * TILE)
            g_t[h, :, cols] = g_s[h, cols, :].T
        return 0

    lax.fori_loop(0, heads, turn_g, 0)

    @pl.when(core == 1)
    def _():
        pl.semaphore_wait(go_sem, 1)
        send_own(0)
        send_own(1)

    def forward_step(step, _):
        for a in range(2):
            take_up(a, step)
            take_dn(a, step)

        @pl.when((core == 0) & (step == GO_AT))
        def _():
            pl.semaphore_signal(go_sem, inc=1, device_id={"cp": peer}, device_id_type=MESH)

        def use(side, _):
            j = jnp.where(side == 0, chip - 1 - step, (chip + 1 + step) % n)
            valid = (j >= 0) & (j < chip) & ((side == 0) | ((j < hops_dn[0]) & (step < hops_dn[0])))

            @pl.when(valid)
            def _():
                forward_chunk(j, False)

            return 0

        lax.fori_loop(0, 2, use, 0)
        return 0

    lax.fori_loop(0, n // 2, forward_step, 0)

    def finish(h, _):
        for i in range(tiles):
            cols = slice(i * TILE, (i + 1) * TILE)
            total = run_l[h, :, cols]
            out = (acc[h, :, cols] / total).astype(jnp.bfloat16)
            acc[h, :, cols] = jnp.zeros((head_dim, TILE), jnp.float32)
            delta[h, :, cols] = jnp.sum(g_t[h, :, cols].astype(jnp.float32) * out.astype(jnp.float32), axis=0, keepdims=True)
            lse2 = run_m[h, :, cols] + jnp.log2(total)
            run_m[h, :, cols] = lse2
            lse_s[h, :, cols] = lse2 * LN2
            by_head[h, cols, :] = out.T
        return 0

    lax.fori_loop(0, heads, finish, 0)
    join_heads(by_head, q_raw)

    def give_back(i, src_mine, src_theirs, dst):
        swap = remote(src_theirs, dst.at[core], back_send.at[i], back_recv.at[i], peer)
        keep = pltpu.make_async_copy(src_mine, dst.at[core], store_sem.at[i])
        swap.start()
        keep.start()
        return swap, keep

    pending = [
        give_back(0, q_raw.at[core], q_raw.at[other], out_hbm),
        give_back(1, lse_s.at[:, :, mine], lse_s.at[:, :, theirs], lse_hbm),
    ]

    def backward_chunk(j, diagonal):
        turn(k_all, j)
        dk_sum[j] = jnp.zeros((chunk, head_dim), jnp.float32)
        dv_sum[j] = jnp.zeros((chunk, head_dim), jnp.float32)

        def head(h, _):
            size = [(i + 1) * TILE if diagonal else chunk for i in range(tiles)]
            cols = [slice(i * TILE, (i + 1) * TILE) for i in range(tiles)]
            ps, dss = [], []
            for i in range(tiles):
                s = jnp.dot(k_all[j, :size[i], :], q_t[h, :, cols[i]], preferred_element_type=jnp.float32)
                dp = jnp.dot(v_all[j, :size[i], :], g_t[h, :, cols[i]], preferred_element_type=jnp.float32)
                if diagonal:
                    s = jnp.where(causal(size[i], i), s, -jnp.inf)
                p = jnp.exp2(s * fold - run_m[h, :, cols[i]])
                ps.append(p.astype(jnp.bfloat16))
                dss.append((p * (dp - delta[h, :, cols[i]])).astype(jnp.bfloat16))
            if diagonal:
                for i in range(tiles):
                    dv_sum[j, :size[i], :] += jnp.dot(ps[i], g_s[h, cols[i], :], preferred_element_type=jnp.float32)
                    dk_sum[j, :size[i], :] += jnp.dot(dss[i], q_s[h, cols[i], :], preferred_element_type=jnp.float32)
                    acc[h, :, cols[i]] += jnp.dot(turned[:, :size[i]], dss[i], preferred_element_type=jnp.float32)
            else:
                pp = jnp.concatenate(ps, axis=1)
                dd = jnp.concatenate(dss, axis=1)
                dv_sum[j] += jnp.dot(pp, g_s[h], preferred_element_type=jnp.float32)
                dk_sum[j] += jnp.dot(dd, q_s[h], preferred_element_type=jnp.float32)
                acc[h] += jnp.dot(turned[...], dd, preferred_element_type=jnp.float32)
            return 0

        lax.fori_loop(0, heads, head, 0, unroll=True)

    def sum_dn(a, step, j):
        return remote(sums[a].at[j], from_up[a].at[step], dkv_dn_send.at[a, step], dkv_dn_recv.at[a, step], below)

    def sum_up(a, step, src):
        return remote(src, from_dn[a].at[step], dkv_up_send.at[a, step], dkv_up_recv.at[a, step], above)

    wide = n // 2
    wrap = False

    def gives_dn(a, step):
        skip = (a == 0) & (step == 0) & (chip == n - 1) & wrap
        return (chip - hops_up[a] + step >= 0) & (step < hops_up[a]) & jnp.logical_not(skip)

    def gets_dn(a, step):
        skip = (a == 0) & (step == 1) & (chip == n - 2) & wrap
        return (step >= 1) & (chip < n - 1) & jnp.logical_not(skip)

    def up_index(step):
        return (chip + wide - step + n) % n

    def gives_up(a, step):
        j = up_index(step)
        in_reach = (j < wide) & (j != chip) & (step < wide)
        if a == 0:
            in_reach &= (wrap & (chip == n - 1)) | ((step >= 1) & (wrap | (j < wide - 1)))
        return in_reach

    def gets_up(a, step):
        return (step >= 2 - a) | ((step >= 1) & (up_index(step) > chip))

    def add_in(a, j, part):
        sums[a][j] = sums[a][j] + part

    def pass_dn(a, step):
        @pl.when(gives_dn(a, step))
        def _():
            j = chip - hops_up[a] + step

            before = jnp.maximum(step - 1, 0)

            @pl.when(gets_dn(a, step))
            def _():
                sum_dn(a, before, j).wait_recv()
                add_in(a, j, from_up[a][before])

            sum_dn(a, step, j).start()

    def pass_up(a, step):
        @pl.when(gives_up(a, step))
        def _():
            j = up_index(step)
            before = jnp.maximum(step - 1, 0)

            @pl.when(gets_up(a, step))
            def _():
                sum_up(a, before, sums[a].at[j]).wait_recv()

            @pl.when(j < chip)
            def _():
                @pl.when(gets_up(a, step))
                def _():
                    add_in(a, j, from_dn[a][before])

                sum_up(a, step, sums[a].at[j]).start()

            @pl.when(j > chip)
            def _():
                sum_up(a, step, from_dn[a].at[before]).start()

    def backward_pos(s, _):
        step = jnp.maximum(s - 1, 0) // 2
        first = s == 0
        down = s % 2 == 1
        near = chip - hops_up[1] + step
        far = up_index(step + 1)
        j = jnp.where(first, chip - n // 2, jnp.where(down, near, far))
        valid = (j >= 0) & (j < chip) & (first | down | (j < wide))

        @pl.when(valid)
        def _():
            backward_chunk(j, False)

        @pl.when(first)
        def _():
            pass_dn(0, 0)
            pass_up(0, 0)
            pass_up(1, 0)

        @pl.when(down)
        def _():
            pass_dn(0, step + 1)
            pass_dn(1, step)

        @pl.when(jnp.logical_not(first | down))
        def _():
            pass_up(0, step + 1)
            pass_up(1, step + 1)

        @pl.when(s == n // 2 - 1)
        def _():
            backward_chunk(chip, True)

        return 0

    lax.fori_loop(0, n - 1, backward_pos, 0)

    def finish_q(h, _):
        for i in range(tiles):
            cols = slice(i * TILE, (i + 1) * TILE)
            by_head[h, cols, :] = (acc[h, :, cols] * scale).astype(jnp.bfloat16).T
        return 0

    lax.fori_loop(0, heads, finish_q, 0)
    join_heads(by_head, g_raw)
    pending.append(give_back(2, g_raw.at[core], g_raw.at[other], dq_hbm))

    for a in range(2):
        @pl.when((chip < wide) if a == 1 else (chip < wide - 1) | (wrap & (chip < wide)))
        def _():
            sum_up(a, wide - 1, sums[a].at[chip]).wait_recv()
            add_in(a, chip, from_dn[a][wide - 1])

        @pl.when(chip < n - 1)
        def _():
            sum_dn(a, hops_up[a] - 1, chip).wait_recv()
            add_in(a, chip, from_up[a][hops_up[a] - 1])

        if a == 0:
            dk_s[...] = (dk_sum[chip] * scale).astype(jnp.bfloat16)
            pending.append(give_back(3, dk_s.at[mine], dk_s.at[theirs], dk_hbm))
        else:
            dv_s[...] = dv_sum[chip].astype(jnp.bfloat16)
            pending.append(give_back(4, dv_s.at[mine], dv_s.at[theirs], dv_hbm))

    for i in range(4):
        swaps[i].wait_send()
    for a in range(2):
        for step in range(hops_up[a]):
            @pl.when(sends_up(a, step))
            def _():
                kv_up(a, step, 0).wait_send()

            @pl.when(gives_dn(a, step))
            def _():
                sum_dn(a, step, 0).wait_send()

        for step in range(hops_dn[a]):
            @pl.when(sends_dn(a, step))
            def _():
                kv_dn(a, step, 0).wait_send()

        for step in range(wide):
            @pl.when(gives_up(a, step))
            def _():
                sum_up(a, step, sums[a].at[0]).wait_send()

    for swap, keep in pending:
        keep.wait()
        swap.wait()


def place_kernel(lse_in, out_in, dq_in, dk_in, dv_in, lse_out, out_out, dq_out, dk_out, dv_out, lse_buf, row_buf, out_buf, dq_buf, dk_buf, dv_buf, in_sem, out_sem):
    pieces = []
    for src, buf, dst in ((out_in, out_buf, out_out), (dq_in, dq_buf, dq_out), (dk_in, dk_buf, dk_out), (dv_in, dv_buf, dv_out)):
        for b in range(src.shape[0]):
            i = len(pieces)
            pieces.append((pltpu.make_async_copy(src.at[b], buf.at[b], in_sem.at[i]), pltpu.make_async_copy(buf.at[b], dst.at[b], out_sem.at[i])))
    last = len(pieces)
    lse_load = pltpu.make_async_copy(lse_in, lse_buf, in_sem.at[last])
    lse_store = pltpu.make_async_copy(row_buf, lse_out, out_sem.at[last])
    lse_load.start()
    for load, _ in pieces:
        load.start()
    lse_load.wait()
    row_buf[...] = lse_buf[:, :, 0, :]
    for load, store in pieces:
        load.wait()
        store.start()
    lse_store.start()
    for _, store in pieces:
        store.wait()
    lse_store.wait()


def solution(mesh):
    chips = mesh.shape["cp"] // 2

    def attention_shard(queries, keys, values, out_grad):
        batch, tokens, heads, head_dim = queries.shape
        chunk = 2 * tokens
        half = chips // 2
        bf16, f32 = jnp.bfloat16, jnp.float32
        k = keys.reshape(batch, tokens, head_dim)
        v = values.reshape(batch, tokens, head_dim)
        any_spec = pl.BlockSpec(memory_space=pl.ANY)
        dma = pltpu.SemaphoreType.DMA
        out, lse, dq, dk, dv = pl.pallas_call(
            functools.partial(attention_kernel, chips, head_dim ** -0.5),
            out_shape=(
                jax.ShapeDtypeStruct(queries.shape, bf16),
                jax.ShapeDtypeStruct((batch, heads, 1, tokens), f32),
                jax.ShapeDtypeStruct(queries.shape, bf16),
                jax.ShapeDtypeStruct(k.shape, bf16),
                jax.ShapeDtypeStruct(k.shape, bf16),
            ),
            in_specs=[any_spec] * 4,
            out_specs=(any_spec,) * 5,
            scratch_shapes=[
                pltpu.VMEM((chips, chunk, head_dim), bf16),
                pltpu.VMEM((chips, chunk, head_dim), bf16),
                pltpu.VMEM((head_dim, chunk), bf16),
                pltpu.VMEM((heads, chunk, head_dim), bf16),
                pltpu.VMEM((heads, head_dim, chunk), bf16),
                pltpu.VMEM((heads, chunk, head_dim), bf16),
                pltpu.VMEM((heads, head_dim, chunk), bf16),
                pltpu.VMEM((heads, head_dim, chunk), f32),
                pltpu.VMEM((heads, 1, chunk), f32),
                pltpu.VMEM((heads, 1, chunk), f32),
                pltpu.VMEM((heads, 1, chunk), f32),
                pltpu.VMEM((heads, 1, chunk), f32),
                pltpu.VMEM((heads, chunk, head_dim), bf16),
                pltpu.VMEM((2, tokens, heads, head_dim), bf16),
                pltpu.VMEM((2, tokens, heads, head_dim), bf16),
                pltpu.VMEM((chunk, head_dim), bf16),
                pltpu.VMEM((chunk, head_dim), bf16),
                pltpu.VMEM((chips, chunk, head_dim), f32),
                pltpu.VMEM((chips, chunk, head_dim), f32),
                pltpu.VMEM((half, chunk, head_dim), f32),
                pltpu.VMEM((half - 1, chunk, head_dim), f32),
                pltpu.VMEM((half, chunk, head_dim), f32),
                pltpu.VMEM((half, chunk, head_dim), f32),
                dma((4,)), dma((4,)), dma((4,)),
                dma((2, half)), dma((2, half)), dma((2, half)), dma((2, half)),
                dma((2, half)), dma((2, half)), dma((2, half)), dma((2, half)),
                dma((5,)), dma((5,)), dma((5,)), pltpu.SemaphoreType.REGULAR,
            ],
            compiler_params=pltpu.CompilerParams(collective_id=0, has_side_effects=True, vmem_limit_bytes=67043328),
            name="ring_attention",
        )(queries, k, v, out_grad)
        results = (out, dq, dk, dv)
        row_lse, out, dq, dk, dv = pl.pallas_call(
            place_kernel,
            out_shape=(jax.ShapeDtypeStruct((batch, heads, tokens), f32),) + tuple(jax.ShapeDtypeStruct(x.shape, bf16) for x in results),
            in_specs=[any_spec] * 5,
            out_specs=(any_spec,) * 5,
            scratch_shapes=[pltpu.VMEM(lse.shape, f32), pltpu.VMEM((batch, heads, tokens), f32)] + [pltpu.VMEM(x.shape, bf16) for x in results] + [dma((4 * batch + 1,))] * 2,
            name="place_results",
        )(lse, *results)
        return out, row_lse, dq, dk.reshape(keys.shape), dv.reshape(values.shape)

    seq_spec = P("dp", "cp")
    return jax.shard_map(attention_shard, mesh=mesh, in_specs=(seq_spec,) * 4, out_specs=(seq_spec, P("dp", None, "cp"), seq_spec, seq_spec, seq_spec), check_vma=False)
```
